32 devices in a mesh: head: 4 (over z), pts: 8 (over y, x, core).
Axes of the slice: x: 2, y: 2, z: 4, core: 2. Of those that a mesh axis runs over, the one named last changes fastest.
Arguments:
- layer_inputs_trainorder: bfloat16 [196608, 256], P(('head', 'pts')), may hold values from -6 to 6
- inference_placement: int32 [196608], P(('head', 'pts')), may hold values from 0 to 196607, as said below
- initial_layernorm_gain: float32 [256], replicated, may hold values from 0.1 to 1.9
- initial_layernorm_offset: float32 [256], replicated, may hold values from -2 to 2
- attribute_projection: bfloat16 [256, 256], replicated, may hold values from -0.375 to 0.375
- assignment_feeder_projection: bfloat16 [256, 256], replicated, may hold values from -0.375 to 0.375
- partition_projection: bfloat16 [16, 32], replicated, may hold values from -1.5 to 1.5
- partition_offset: float32 [32], replicated, may hold values from -4 to 4
- softmax_sharpness: float32 [16], P('head'), may hold values from 0.03 to 1
- partition_question_map: float32 [16, 16], replicated, may hold values from -1.5 to 1.5
- partition_lookup_map: float32 [16, 16], replicated, may hold values from -1.5 to 1.5
- partition_content_map: float32 [16, 16], replicated, may hold values from -1.5 to 1.5
- emitted_projection: bfloat16 [256, 256], replicated, may hold values from -0.375 to 0.375
- emitted_offset: float32 [256], replicated, may hold values from -2 to 2
- latter_layernorm_gain: float32 [256], replicated, may hold values from 0.1 to 1.9
- latter_layernorm_offset: float32 [256], replicated, may hold values from -2 to 2
- perceptron_entry_map: bfloat16 [256, 1024], replicated, may hold values from -0.375 to 0.375
- perceptron_entry_offset: float32 [1024], replicated, may hold values from -2 to 2
- perceptron_exit_map: bfloat16 [1024, 256], replicated, may hold values from -0.1875 to 0.1875
- perceptron_exit_offset: float32 [256], replicated, may hold values from -2 to 2
Outputs:
- served: bfloat16 [8, 24576, 256], P('pts', 'head')
The draws below stay inside these ranges and needn't reach their ends.
Inputs may be any that keep to these rules, and one draw needn't show every extreme that they name: inference_placement is a permutation of all points; of the 6144 points of each aligned block of the training order, exactly 192 go to each aligned block of 6144 serving positions.
All inputs are finite; a program needn't handle non-finite values.
Results may differ from the reference program's by a relative error of at most 0.0035.
The reference program's roundings to bfloat16 on the way count: a program that leaves them out, or rounds other values in their place, can miss the bound.
Values may be sent and summed in bfloat16 or wider, within the bound.
No kernel may reach another device: no remote copies, remote signals or barrier semaphores. Data moves between devices by JAX's collectives and lax.ppermute only.
A program may use at most 128 MiB of HBM per device.

```python
import math
import jax
import jax.numpy as jnp
from jax import lax

ATTENDER_TOTAL = 16
DH = 16
M = 32
FF = 1024
PTS_DEV = 6144
MODEL_CHANNELS = 256
SERVE = 24576
POINTS = 196608
N_PTS = 8


def draw_inference_placement(key, part):
    blocks = POINTS // PTS_DEV
    per_pair = PTS_DEV // blocks
    first_keys = jax.random.split(jax.random.fold_in(key, 11), blocks)
    second_keys = jax.random.split(jax.random.fold_in(key, 12), blocks)
    within = jax.vmap(lambda single: jax.random.permutation(single, PTS_DEV))(first_keys).astype(jnp.int32)
    arrival = jax.vmap(lambda single: jax.random.permutation(single, PTS_DEV))(second_keys).astype(jnp.int32)
    target = within // per_pair
    ranks_in = within % per_pair
    source_ids = jnp.arange(blocks, dtype=jnp.int32)[:, None]
    slot_ids = source_ids * per_pair + ranks_in
    positions = target * PTS_DEV + arrival[target, slot_ids]
    return positions.reshape(-1).astype(jnp.int32)


def level_of(key, shape, cuts, smallest, high):
    loudness, own = 1.0, jax.random.fold_in(key, 6)
    for axis_at, parts in cuts:
        steps = jnp.exp(jax.random.uniform(jax.random.fold_in(own, axis_at), (parts,), jnp.float32, smallest / len(cuts), high / len(cuts)))
        loudness = loudness * jnp.repeat(steps, shape[axis_at] // parts).reshape([-1 if axis == axis_at else 1 for axis in range(len(shape))])
    return loudness


def bell_draw(stream_key, shape, deviation, bound, cuts=(), held_as=jnp.bfloat16):
    loudness = level_of(stream_key, shape, cuts, -0.22, 0.18) if cuts else 1.0
    result = jax.random.normal(stream_key, shape, jnp.float32) * deviation * loudness
    return jnp.minimum(jnp.maximum(result, -bound), bound).astype(held_as)


def setup_inputs(seed: int = 0) -> dict:
    key_of = jax.random.split(jax.random.key(seed), 21)
    return {
        "layer_inputs_trainorder": bell_draw(key_of[0], (POINTS, MODEL_CHANNELS), 1.0, 6.0, ((0, 32),)),
        "inference_placement": draw_inference_placement(jax.random.fold_in(key_of[20], 71), 0),
        "initial_layernorm_gain": jnp.clip(1.0 + 0.18 * jax.random.normal(key_of[2], (MODEL_CHANNELS,), jnp.float32), 0.1, 1.9),
        "initial_layernorm_offset": bell_draw(key_of[3], (MODEL_CHANNELS,), 0.3, 2.0, (), jnp.float32),
        "attribute_projection": bell_draw(key_of[4], (MODEL_CHANNELS, MODEL_CHANNELS), MODEL_CHANNELS ** -0.5, 0.375),
        "assignment_feeder_projection": bell_draw(key_of[5], (MODEL_CHANNELS, MODEL_CHANNELS), MODEL_CHANNELS ** -0.5, 0.375),
        "partition_projection": bell_draw(key_of[6], (DH, M), DH ** -0.5, 1.5),
        "partition_offset": bell_draw(key_of[7], (M,), 1.0, 4.0, (), jnp.float32),
        "softmax_sharpness": jnp.clip(jnp.exp(math.log(1.0) - 3.506558 * jax.random.uniform(key_of[8], (ATTENDER_TOTAL,), jnp.float32) ** level_of(key_of[8], (ATTENDER_TOTAL,), ((0, 4),), -0.2, 0.2)), 0.03, 1.0),
        "partition_question_map": bell_draw(key_of[9], (DH, DH), DH ** -0.5, 1.5, (), jnp.float32),
        "partition_lookup_map": bell_draw(key_of[10], (DH, DH), DH ** -0.5, 1.5, (), jnp.float32),
        "partition_content_map": bell_draw(key_of[11], (DH, DH), DH ** -0.5, 1.5, (), jnp.float32),
        "emitted_projection": bell_draw(key_of[12], (MODEL_CHANNELS, MODEL_CHANNELS), MODEL_CHANNELS ** -0.5, 0.375),
        "emitted_offset": bell_draw(key_of[13], (MODEL_CHANNELS,), 0.3, 2.0, (), jnp.float32),
        "latter_layernorm_gain": jnp.clip(1.0 + 0.18 * jax.random.normal(key_of[14], (MODEL_CHANNELS,), jnp.float32), 0.1, 1.9),
        "latter_layernorm_offset": bell_draw(key_of[15], (MODEL_CHANNELS,), 0.3, 2.0, (), jnp.float32),
        "perceptron_entry_map": bell_draw(key_of[16], (MODEL_CHANNELS, FF), MODEL_CHANNELS ** -0.5, 0.375),
        "perceptron_entry_offset": bell_draw(key_of[17], (FF,), 0.3, 2.0, (), jnp.float32),
        "perceptron_exit_map": bell_draw(key_of[18], (FF, MODEL_CHANNELS), FF ** -0.5, 0.1875),
        "perceptron_exit_offset": bell_draw(key_of[19], (MODEL_CHANNELS,), 0.3, 2.0, (), jnp.float32),
    }


def layer_norm(row_block, gain_vec, bias_vec):
    row_mean = lax.optimization_barrier(jnp.mean(row_block, axis=-1, keepdims=True))
    centred = row_block - row_mean
    spread = lax.optimization_barrier(jnp.mean(centred * centred, axis=-1, keepdims=True))
    return centred * lax.rsqrt(spread + 1e-05) * gain_vec + bias_vec

def truncated_coefficients(value):
    return lax.optimization_barrier(value.astype(jnp.bfloat16)).astype(jnp.float32)

def partition_share_entries(standardized_entries, assignment_feeder_projection, partition_projection, partition_offset, softmax_sharpness):
    middle = truncated_coefficients(jnp.dot(standardized_entries, assignment_feeder_projection, preferred_element_type=jnp.float32)).reshape(-1, ATTENDER_TOTAL, DH)
    partition_scores_raw = jnp.einsum('rhd,dm->rhm', middle, partition_projection.astype(jnp.float32))
    partition_scores_raw = (partition_scores_raw + partition_offset) / softmax_sharpness[:, None]
    return jax.nn.softmax(partition_scores_raw, axis=-1)

def reference(layer_inputs_trainorder, inference_placement, initial_layernorm_gain, initial_layernorm_offset, attribute_projection, assignment_feeder_projection, partition_projection, partition_offset, softmax_sharpness, partition_question_map, partition_lookup_map, partition_content_map, emitted_projection, emitted_offset, latter_layernorm_gain, latter_layernorm_offset, perceptron_entry_map, perceptron_entry_offset, perceptron_exit_map, perceptron_exit_offset):
    block_count = POINTS // PTS_DEV
    row_blocks = layer_inputs_trainorder.reshape(block_count, PTS_DEV, MODEL_CHANNELS)

    def gather_sums(running_state, row_block):
        standardized_entries = layer_norm(row_block.astype(jnp.float32), initial_layernorm_gain, initial_layernorm_offset).astype(jnp.bfloat16)
        slice_feature_rows = truncated_coefficients(jnp.dot(standardized_entries, attribute_projection, preferred_element_type=jnp.float32)).reshape(-1, ATTENDER_TOTAL, DH)
        coefficient_array = partition_share_entries(standardized_entries, assignment_feeder_projection, partition_projection, partition_offset, softmax_sharpness)
        coefficients_halfprecision = truncated_coefficients(coefficient_array)
        return ((running_state[0] + lax.optimization_barrier(jnp.sum(coefficient_array, axis=0)), running_state[1] + jnp.einsum('qct,qcv->ctv', coefficients_halfprecision, slice_feature_rows)), None)
    start = (jnp.zeros((ATTENDER_TOTAL, M), jnp.float32), jnp.zeros((ATTENDER_TOTAL, M, DH), jnp.float32))
    (totals, numerator), unused = lax.scan(gather_sums, start, row_blocks)
    slice_token = numerator / (totals + 1e-05)[:, :, None]
    highest_mode = lax.Precision.HIGHEST
    query_rows = jnp.einsum('izn,nu->izu', slice_token, partition_question_map, precision=highest_mode)
    key_vectors = jnp.einsum('izn,nu->izu', slice_token, partition_lookup_map, precision=highest_mode)
    value_rows = jnp.einsum('izn,nu->izu', slice_token, partition_content_map, precision=highest_mode)
    score_scale = 1.0 / math.sqrt(DH)
    scores = jnp.einsum('hme,hne->hmn', query_rows, key_vectors, precision=highest_mode) * score_scale
    attention = jax.nn.softmax(scores, axis=-1)
    slice_output = truncated_coefficients(jnp.einsum('hmn,hne->hme', attention, value_rows, precision=highest_mode))
    inverse = jnp.argsort(inference_placement).astype(jnp.int32).reshape(block_count, PTS_DEV)

    def serve_block(serve_index):
        row_block = jnp.take(layer_inputs_trainorder, serve_index, axis=0)
        standardized_entries = layer_norm(row_block.astype(jnp.float32), initial_layernorm_gain, initial_layernorm_offset).astype(jnp.bfloat16)
        coefficients_halfprecision = truncated_coefficients(partition_share_entries(standardized_entries, assignment_feeder_projection, partition_projection, partition_offset, softmax_sharpness))
        blended_rows = jnp.einsum('fny,nyp->fnp', coefficients_halfprecision, slice_output).astype(jnp.bfloat16).reshape(-1, MODEL_CHANNELS)
        hidden = row_block.astype(jnp.float32) + jnp.dot(blended_rows, emitted_projection, preferred_element_type=jnp.float32) + emitted_offset
        normed_two = layer_norm(hidden, latter_layernorm_gain, latter_layernorm_offset).astype(jnp.bfloat16)
        inner_act = jax.nn.gelu(jnp.dot(normed_two, perceptron_entry_map, preferred_element_type=jnp.float32) + perceptron_entry_offset, approximate=False).astype(jnp.bfloat16)
        return (hidden + jnp.dot(inner_act, perceptron_exit_map, preferred_element_type=jnp.float32) + perceptron_exit_offset).astype(jnp.bfloat16)
    served = lax.map(serve_block, inverse)
    return served.reshape(N_PTS, SERVE, MODEL_CHANNELS)
```

```python
import functools
import math

import jax
import jax.numpy as jnp
from jax import lax
from jax.experimental import pallas as pl
from jax.experimental.pallas import tpu as pltpu
from jax.sharding import PartitionSpec as P

F32 = jnp.float32
BF16 = jnp.bfloat16
LANES = 128
TAIL = 8
EPS_NORM = 1e-05
LOG2E = math.log2(math.e)
NT = (((1,), (1,)), ((), ()))
TN = (((0,), (0,)), ((), ()))
VMEM = 56 * 1024 * 1024


def whole(shape):
    return pl.BlockSpec(shape, lambda *_: (0,) * len(shape))


def params():
    return pltpu.CompilerParams(vmem_limit_bytes=VMEM)


def floor_div(value, divisor):
    return jnp.floor((value + 0.5) * (1.0 / divisor))


def norm_rows(row_block, gain, bias):
    mean = jnp.mean(row_block, axis=-1, keepdims=True)
    centred = row_block - mean
    spread = jnp.mean(centred * centred, axis=-1, keepdims=True)
    return centred * lax.rsqrt(spread + EPS_NORM) * gain + bias


def rank_kernel(place_ref, pos_ref, tail_ref, hot_ref, count_ref, key_ref, *, local, groups, shards, per):
    devices = groups * shards
    chunks = place_ref.shape[0]
    placement = place_ref[...].astype(F32)
    block = floor_div(placement, local)
    within = placement - block * local
    outer = floor_div(block, groups)
    target = (block - outer * groups) * shards + outer
    high = floor_div(within, LANES)
    low = within - high * LANES
    ids = lax.broadcasted_iota(jnp.int32, (devices, LANES), 0).astype(F32)
    for c in range(chunks):
        hot = (ids == target[c : c + 1, :]).astype(F32)
        hot_ref[:, c * LANES : (c + 1) * LANES] = hot.astype(BF16)
    before = lax.broadcasted_iota(jnp.int32, (LANES, LANES), 0) < lax.broadcasted_iota(
        jnp.int32, (LANES, LANES), 1
    )
    prefix = jnp.concatenate(
        [before.astype(F32), jnp.ones((LANES, LANES), F32)], axis=1
    ).astype(BF16)
    for c in range(chunks):
        count_ref[c * devices : (c + 1) * devices, :] = jnp.dot(
            hot_ref[:, c * LANES : (c + 1) * LANES], prefix, preferred_element_type=F32
        )
    carry = jnp.zeros((devices, LANES), F32)
    slots = lax.broadcasted_iota(jnp.int32, (per, LANES), 0).astype(F32)
    for c in range(chunks):
        counts = count_ref[c * devices : (c + 1) * devices, :]
        hot = hot_ref[:, c * LANES : (c + 1) * LANES].astype(F32)
        rank = jnp.sum(hot * (counts[:, :LANES] + carry), axis=0, keepdims=True)
        carry = carry + counts[:, LANES:]
        pos_ref[c : c + 1, :] = (target[c : c + 1, :] * per + rank).astype(jnp.int32)
        chosen = slots == rank
        key_ref[:per, c * LANES : (c + 1) * LANES] = jnp.where(
            chosen, high[c : c + 1, :], 0.0
        ).astype(BF16)
        key_ref[per:, c * LANES : (c + 1) * LANES] = jnp.where(
            chosen, low[c : c + 1, :], 0.0
        ).astype(BF16)
    tail_ref[...] = lax.dot_general(
        hot_ref[...], key_ref[...], NT, preferred_element_type=F32
    ).astype(BF16)


def rank_rows(placement, local, groups, shards):
    devices = groups * shards
    per = local // devices
    chunks = local // LANES
    return pl.pallas_call(
        functools.partial(rank_kernel, local=local, groups=groups, shards=shards, per=per),
        out_shape=(
            jax.ShapeDtypeStruct((chunks, LANES), jnp.int32),
            jax.ShapeDtypeStruct((devices, 2 * per), BF16),
        ),
        scratch_shapes=[
            pltpu.VMEM((devices, local), BF16),
            pltpu.VMEM((chunks * devices, 2 * LANES), F32),
            pltpu.VMEM((2 * per, local), BF16),
        ],
        compiler_params=params(),
        name="rank_rows",
    )(placement.reshape(chunks, LANES))


def scatter_kernel(pos_ref, x_ref, tail_ref, out_ref, src_lo, src_hi, dst_lo, dst_hi, *, per):
    chunks = pos_ref.shape[0]
    devices = tail_ref.shape[0]

    def widen(c, carry):
        rows = pl.ds(pl.multiple_of(c * LANES, LANES), LANES)
        src_lo[rows, :] = x_ref[rows, :LANES].astype(F32)
        src_hi[rows, :] = x_ref[rows, LANES:].astype(F32)
        return carry

    lax.fori_loop(0, chunks, widen, 0)

    def move(c, carry):
        base = c * LANES
        for j in range(LANES):
            slot = pos_ref[c, j]
            dst_lo[pl.ds(slot, 1), :] = src_lo[pl.ds(base + j, 1), :]
            dst_hi[pl.ds(slot, 1), :] = src_hi[pl.ds(base + j, 1), :]
        return carry

    lax.fori_loop(0, chunks, move, 0)

    def narrow(d, carry):
        rows = pl.ds(pl.multiple_of(d * per, 16), per)
        out_ref[d, :per, :LANES] = dst_lo[rows, :].astype(BF16)
        out_ref[d, :per, LANES:] = dst_hi[rows, :].astype(BF16)
        return carry

    lax.fori_loop(0, devices, narrow, 0)
    out_ref[:, per:, :] = tail_ref[...]


def scatter_rows(positions, rows, tail, per):
    local, width = rows.shape
    devices = tail.shape[0]
    return pl.pallas_call(
        functools.partial(scatter_kernel, per=per),
        in_specs=[
            pl.BlockSpec(memory_space=pltpu.SMEM),
            pl.BlockSpec(memory_space=pltpu.VMEM),
            pl.BlockSpec(memory_space=pltpu.VMEM),
        ],
        out_shape=jax.ShapeDtypeStruct((devices, per + TAIL, width), BF16),
        scratch_shapes=[pltpu.VMEM((local, LANES), F32)] * 4,
        compiler_params=params(),
        name="scatter_rows",
    )(positions, rows, tail)


def slice_weights(standard, feeder_t, logit_t, sharp_ref, offset_ref, logit_ref, weight_ref, total_ref):
    heads = sharp_ref.shape[0]
    slices = offset_ref.shape[1]
    middle = lax.dot_general(feeder_t[...], standard, NT, preferred_element_type=F32).astype(BF16)
    logit_ref[...] = jnp.dot(logit_t[...], middle, preferred_element_type=F32)
    sharp = sharp_ref[...]

    def column(c, carry):
        lanes = pl.ds(pl.multiple_of(c * LANES, LANES), LANES)
        top = None
        for m in range(slices):
            value = (logit_ref[m * heads : (m + 1) * heads, lanes] + offset_ref[0, m]) * sharp
            top = value if top is None else jnp.maximum(top, value)
        total = None
        for m in range(slices):
            value = (logit_ref[m * heads : (m + 1) * heads, lanes] + offset_ref[0, m]) * sharp
            value = jnp.exp2(value - top)
            logit_ref[m * heads : (m + 1) * heads, lanes] = value
            total = value if total is None else total + value
        scale = 1.0 / total
        for m in range(slices):
            value = logit_ref[m * heads : (m + 1) * heads, lanes] * scale
            weight_ref[m * heads : (m + 1) * heads, lanes] = value.astype(BF16)
            if total_ref is not None:
                total_ref[m * heads : (m + 1) * heads, :] += value
        return carry

    lax.fori_loop(0, weight_ref.shape[1] // LANES, column, 0)


def sums_kernel(
    x_ref, gain, bias, attribute, feeder_t, logit_t, sharp_ref, offset_ref,
    packed_ref, logit_ref, weight_ref, total_ref, numer_ref,
):
    step = pl.program_id(0)
    heads = sharp_ref.shape[0]
    rows, width = numer_ref.shape
    feature = width // heads

    @pl.when(step == 0)
    def _():
        total_ref[...] = jnp.zeros_like(total_ref)
        numer_ref[...] = jnp.zeros_like(numer_ref)

    standard = norm_rows(x_ref[...].astype(F32), gain[...], bias[...]).astype(BF16)
    features = jnp.dot(standard, attribute[...], preferred_element_type=F32).astype(BF16)
    slice_weights(
        standard, feeder_t, logit_t, sharp_ref, offset_ref, logit_ref, weight_ref, total_ref
    )
    numer_ref[...] += jnp.dot(weight_ref[...], features, preferred_element_type=F32)

    @pl.when(step == pl.num_programs(0) - 1)
    def _():
        row_head = lax.broadcasted_iota(jnp.int32, (rows, width), 0) % heads
        column_head = lax.broadcasted_iota(jnp.int32, (rows, width), 1) // feature
        own = jnp.where(row_head == column_head, numer_ref[...], 0.0)
        folded = own[:, :LANES]
        for start in range(LANES, width, LANES):
            folded = folded + own[:, start : start + LANES]
        shift = LANES // 2
        while shift >= feature:
            folded = folded + pltpu.roll(folded, shift, 1)
            shift //= 2
        pack = LANES // feature
        sub = lax.broadcasted_iota(jnp.int32, (rows, LANES), 0) % pack
        lane = lax.broadcasted_iota(jnp.int32, (rows, LANES), 1) // feature
        packed = jnp.where(sub == lane, folded, 0.0).reshape(rows // pack, pack, LANES)
        packed_ref[: rows // pack, :] = jnp.sum(packed, axis=1)
        sums = jnp.sum(total_ref[...], axis=1, keepdims=True)
        sub = lax.broadcasted_iota(jnp.int32, (rows, LANES), 0) % LANES
        lane = lax.broadcasted_iota(jnp.int32, (rows, LANES), 1)
        packed = jnp.where(sub == lane, sums, 0.0).reshape(rows // LANES, LANES, LANES)
        packed_ref[rows // pack :, :] = jnp.sum(packed, axis=1)


def local_sums(x, gain, bias, attribute, feeder_t, logit_t, sharp, offset, block):
    local, width = x.shape
    rows = logit_t.shape[0]
    heads = sharp.shape[0]
    feature = width // heads
    height = rows * feature // LANES + rows // LANES
    return pl.pallas_call(
        sums_kernel,
        grid=(local // block,),
        in_specs=[
            pl.BlockSpec((block, width), lambda i: (i, 0)),
            whole(gain.shape), whole(bias.shape), whole(attribute.shape), whole(feeder_t.shape),
            whole(logit_t.shape), whole(sharp.shape),
            pl.BlockSpec(memory_space=pltpu.SMEM),
        ],
        out_specs=whole((height, LANES)),
        out_shape=jax.ShapeDtypeStruct((height, LANES), F32),
        scratch_shapes=[
            pltpu.VMEM((rows, block), F32),
            pltpu.VMEM((rows, block), BF16),
            pltpu.VMEM((rows, LANES), F32),
            pltpu.VMEM((rows, width), F32),
        ],
        compiler_params=params(),
        cost_estimate=pl.CostEstimate(flops=5_000_000_000, bytes_accessed=4_000_000, transcendentals=3_000_000),
        name="local_sums",
    )(x, gain, bias, attribute, feeder_t, logit_t, sharp, offset)


def finish_kernel(
    pos_ref, x_ref, gain, bias, feeder_t, logit_t, sharp_ref, offset_ref, mix_t, emitted, emitted_offset,
    gain2, bias2, entry, entry_offset, leave, leave_offset,
    out_ref, logit_ref, weight_ref, res_lo, res_hi, dst_lo, dst_hi, *, per,
):
    step = pl.program_id(0)
    sources = x_ref.shape[0]
    x = jnp.concatenate([x_ref[s, :per, :] for s in range(sources)], axis=0).astype(F32)
    standard = norm_rows(x, gain[...], bias[...]).astype(BF16)
    slice_weights(standard, feeder_t, logit_t, sharp_ref, offset_ref, logit_ref, weight_ref, None)
    blended_t = jnp.dot(mix_t[...], weight_ref[...], preferred_element_type=F32)
    blended = blended_t.T.astype(BF16)
    hidden = x + jnp.dot(blended, emitted[...], preferred_element_type=F32) + emitted_offset[...]
    normed = norm_rows(hidden, gain2[...], bias2[...]).astype(BF16)
    inner = jnp.dot(normed, entry[...], preferred_element_type=F32) + entry_offset[...]
    active = (0.5 * inner * (1.0 + lax.erf(inner * math.sqrt(0.5)))).astype(BF16)
    result = hidden + jnp.dot(active, leave[...], preferred_element_type=F32) + leave_offset[...]
    res_lo[...] = result[:, :LANES]
    res_hi[...] = result[:, LANES:]

    unit = 16

    def move(i, carry):
        for j in range(unit):
            row = i * unit + j
            slot = pos_ref[step, row]
            dst_lo[pl.ds(slot, 1), :] = res_lo[pl.ds(row, 1), :]
            dst_hi[pl.ds(slot, 1), :] = res_hi[pl.ds(row, 1), :]
        return carry

    lax.fori_loop(0, sources * per // unit, move, 0)

    @pl.when(step == pl.num_programs(0) - 1)
    def _():
        def narrow(c, carry):
            rows = pl.ds(pl.multiple_of(c * LANES, LANES), LANES)
            out_ref[rows, :LANES] = dst_lo[rows, :].astype(BF16)
            out_ref[rows, LANES:] = dst_hi[rows, :].astype(BF16)
            return carry

        lax.fori_loop(0, out_ref.shape[0] // LANES, narrow, 0)


def finish_rows(positions, arrived, gain, bias, feeder_t, logit_t, sharp, offset, mix_t, rest, per, sources):
    devices, stride, width = arrived.shape
    local = devices * per
    rows = logit_t.shape[0]
    block = sources * per
    weights = (gain, bias, feeder_t, logit_t, sharp)
    return pl.pallas_call(
        functools.partial(finish_kernel, per=per),
        grid=(devices // sources,),
        in_specs=[
            pl.BlockSpec(memory_space=pltpu.SMEM),
            pl.BlockSpec((sources, stride, width), lambda i: (i, 0, 0)),
            *[whole(w.shape) for w in weights],
            pl.BlockSpec(memory_space=pltpu.SMEM),
            whole(mix_t.shape),
            *[whole(w.shape) for w in rest],
        ],
        out_specs=whole((local, width)),
        out_shape=jax.ShapeDtypeStruct((local, width), BF16),
        scratch_shapes=[
            pltpu.VMEM((rows, block), F32),
            pltpu.VMEM((rows, block), BF16),
            pltpu.VMEM((block, LANES), F32),
            pltpu.VMEM((block, LANES), F32),
            pltpu.VMEM((local, LANES), F32),
            pltpu.VMEM((local, LANES), F32),
        ],
        compiler_params=params(),
        name="finish_rows",
    )(positions, arrived, *weights, offset, mix_t, *rest)


def sum_devices(value, devices):
    step = 1
    while step < devices:
        value = value + lax.ppermute(
            value, ("head", "pts"), [(i, i ^ step) for i in range(devices)]
        )
        step *= 2
    return value


def slice_attention(totals, numerator, question, lookup, content):
    token = numerator / (totals + 1e-05)[:, :, None]
    highest = lax.Precision.HIGHEST
    query = jnp.einsum("izn,nu->izu", token, question, precision=highest)
    key = jnp.einsum("izn,nu->izu", token, lookup, precision=highest)
    value = jnp.einsum("izn,nu->izu", token, content, precision=highest)
    scale = 1.0 / math.sqrt(question.shape[0])
    scores = jnp.einsum("hme,hne->hmn", query, key, precision=highest) * scale
    attention = jax.nn.softmax(scores, axis=-1)
    return jnp.einsum("hmn,hne->hme", attention, value, precision=highest).astype(BF16)


def body(
    layer_inputs_trainorder,
    inference_placement,
    initial_layernorm_gain,
    initial_layernorm_offset,
    attribute_projection,
    assignment_feeder_projection,
    partition_projection,
    partition_offset,
    softmax_sharpness,
    partition_question_map,
    partition_lookup_map,
    partition_content_map,
    emitted_projection,
    emitted_offset,
    latter_layernorm_gain,
    latter_layernorm_offset,
    perceptron_entry_map,
    perceptron_entry_offset,
    perceptron_exit_map,
    perceptron_exit_offset,
):
    groups = lax.axis_size("head")
    shards = lax.axis_size("pts")
    devices = groups * shards
    local, width = layer_inputs_trainorder.shape
    feature, slices = partition_projection.shape
    heads = width // feature
    per = local // devices
    block = 768 if local % 768 == 0 else LANES
    sources = max(1, block // per)

    own = softmax_sharpness.shape[0]
    place = lax.axis_index("head")
    sharpness = jnp.zeros((groups, own), F32)
    sharpness = lax.dynamic_update_slice(sharpness, softmax_sharpness[None], (place, 0))
    step = 1
    while step < groups:
        sharpness = sharpness + lax.ppermute(
            sharpness, "head", [(i, i ^ step) for i in range(groups)]
        )
        step *= 2
    sharp = jnp.broadcast_to((LOG2E / sharpness.reshape(heads))[:, None], (heads, LANES))

    positions, tail = rank_rows(inference_placement, local, groups, shards)
    tail = jnp.pad(tail.reshape(devices, 2, per), ((0, 0), (0, TAIL - 2), (0, width - per)))
    ordered = scatter_rows(positions, layer_inputs_trainorder, tail, per)
    arrived = lax.all_to_all(ordered, ("head", "pts"), split_axis=0, concat_axis=0, tiled=True)
    codes = arrived[:, per : per + 2, :per].astype(F32)
    arrived_at = (codes[:, 0] * LANES + codes[:, 1]).astype(jnp.int32)
    arrived_at = arrived_at.reshape(devices // sources, sources * per)

    gain = initial_layernorm_gain[None]
    bias = initial_layernorm_offset[None]
    feeder_t = assignment_feeder_projection.T
    same = jnp.eye(heads, dtype=BF16)
    logit_t = (
        partition_projection.T[:, None, None, :] * same[None, :, :, None]
    ).reshape(slices * heads, width)
    offset = partition_offset[None]

    packed = local_sums(
        layer_inputs_trainorder, gain, bias, attribute_projection, feeder_t, logit_t, sharp, offset, block
    )
    packed = sum_devices(packed, devices)
    split = slices * heads * feature // LANES
    numerator = packed[:split].reshape(slices, heads, feature).transpose(1, 0, 2)
    totals = packed[split:].reshape(slices, heads).T
    mixed = slice_attention(
        totals, numerator, partition_question_map, partition_lookup_map, partition_content_map
    )
    mix_t = (
        mixed.transpose(0, 2, 1)[:, :, :, None] * same[:, None, None, :]
    ).reshape(width, slices * heads)
    rest = (
        emitted_projection, emitted_offset[None], latter_layernorm_gain[None], latter_layernorm_offset[None],
        perceptron_entry_map, perceptron_entry_offset[None], perceptron_exit_map, perceptron_exit_offset[None],
    )
    served = finish_rows(
        arrived_at, arrived, gain, bias, feeder_t, logit_t, sharp, offset, mix_t, rest, per, sources
    )
    return served[None]


def solution(mesh):
    rows = P(("head", "pts"))
    placed = (P(("head", "pts"), None), rows, *[P()] * 6, P("head"), *[P()] * 11)
    return jax.shard_map(
        body, mesh=mesh, in_specs=placed, out_specs=P("pts", "head", None), check_vma=False
    )
```

```python
import functools
import math

import jax
import jax.numpy as jnp
from jax import lax
from jax.experimental import pallas as pl
from jax.experimental.pallas import tpu as pltpu
from jax.sharding import PartitionSpec as P

F32 = jnp.float32
BF16 = jnp.bfloat16
LANES = 128
TAIL = 8
EPS_NORM = 1e-05
LOG2E = math.log2(math.e)
NT = (((1,), (1,)), ((), ()))
TN = (((0,), (0,)), ((), ()))
VMEM = 56 * 1024 * 1024


def whole(shape):
    return pl.BlockSpec(shape, lambda *_: (0,) * len(shape))


def params():
    return pltpu.CompilerParams(vmem_limit_bytes=VMEM)


def floor_div(value, divisor):
    return jnp.floor((value + 0.5) * (1.0 / divisor))


def norm_rows(row_block, gain, bias):
    mean = jnp.mean(row_block, axis=-1, keepdims=True)
    centred = row_block - mean
    spread = jnp.mean(centred * centred, axis=-1, keepdims=True)
    return centred * lax.rsqrt(spread + EPS_NORM) * gain + bias


def rank_kernel(place_ref, pos_ref, tail_ref, hot_ref, count_ref, key_ref, *, local, groups, shards, per):
    devices = groups * shards
    chunks = place_ref.shape[0]
    placement = place_ref[...].astype(F32)
    block = floor_div(placement, local)
    within = placement - block * local
    outer = floor_div(block, groups)
    target = (block - outer * groups) * shards + outer
    high = floor_div(within, LANES)
    low = within - high * LANES
    ids = lax.broadcasted_iota(jnp.int32, (devices, LANES), 0).astype(F32)
    for c in range(chunks):
        hot = (ids == target[c : c + 1, :]).astype(F32)
        hot_ref[:, c * LANES : (c + 1) * LANES] = hot.astype(BF16)
    before = lax.broadcasted_iota(jnp.int32, (LANES, LANES), 0) < lax.broadcasted_iota(
        jnp.int32, (LANES, LANES), 1
    )
    prefix = jnp.concatenate(
        [before.astype(F32), jnp.ones((LANES, LANES), F32)], axis=1
    ).astype(BF16)
    for c in range(chunks):
        count_ref[c * devices : (c + 1) * devices, :] = jnp.dot(
            hot_ref[:, c * LANES : (c + 1) * LANES], prefix, preferred_element_type=F32
        )
    carry = jnp.zeros((devices, LANES), F32)
    padded = key_ref.shape[0] // 2
    slots = lax.broadcasted_iota(jnp.int32, (padded, LANES), 0).astype(F32)
    for c in range(chunks):
        counts = count_ref[c * devices : (c + 1) * devices, :]
        hot = hot_ref[:, c * LANES : (c + 1) * LANES].astype(F32)
        rank = jnp.sum(hot * (counts[:, :LANES] + carry), axis=0, keepdims=True)
        carry = carry + counts[:, LANES:]
        pos_ref[c : c + 1, :] = (target[c : c + 1, :] * per + rank).astype(jnp.int32)
        chosen = slots == rank
        key_ref[:padded, c * LANES : (c + 1) * LANES] = jnp.where(
            chosen, high[c : c + 1, :], 0.0
        ).astype(BF16)
        key_ref[padded:, c * LANES : (c + 1) * LANES] = jnp.where(
            chosen, low[c : c + 1, :], 0.0
        ).astype(BF16)
    codes = lax.dot_general(hot_ref[...], key_ref[...], NT, preferred_element_type=F32)
    tail_ref[...] = jnp.zeros_like(tail_ref)
    tail_ref[:devices, :padded] = codes[:, :padded]
    tail_ref[devices:, :padded] = codes[:, padded:]


def rank_rows(placement, local, width, groups, shards):
    devices = groups * shards
    per = local // devices
    padded = -(-per // LANES) * LANES
    chunks = local // LANES
    return pl.pallas_call(
        functools.partial(rank_kernel, local=local, groups=groups, shards=shards, per=per),
        out_shape=(
            jax.ShapeDtypeStruct((chunks, LANES), jnp.int32),
            jax.ShapeDtypeStruct((2 * devices, width), F32),
        ),
        scratch_shapes=[
            pltpu.VMEM((devices, local), BF16),
            pltpu.VMEM((chunks * devices, 2 * LANES), F32),
            pltpu.VMEM((2 * padded, local), BF16),
        ],
        compiler_params=params(),
        name="rank_rows",
    )(placement.reshape(chunks, LANES))


def move_rows(slots_ref, first, source_ref, start, target_ref, count):
    source_half = source_ref.shape[0] // 2
    target_half = target_ref.shape[0] // 2
    for j in range(count):
        slot = slots_ref[first + j]
        target_ref[pl.ds(slot, 1), :] = source_ref[pl.ds(start + j, 1), :]
        target_ref[pl.ds(slot + target_half, 1), :] = source_ref[pl.ds(start + (source_half + j), 1), :]


def scatter_kernel(pos_ref, x_ref, tail_ref, out_ref, src, dst, *, per):
    local = x_ref.shape[0]
    devices = tail_ref.shape[0] // 2

    def widen(c, carry):
        first = pl.multiple_of(c * LANES, LANES)
        src[pl.ds(first, LANES), :] = x_ref[pl.ds(first, LANES), :LANES].astype(F32)
        src[pl.ds(first + local, LANES), :] = x_ref[pl.ds(first, LANES), LANES:].astype(F32)
        return carry

    lax.fori_loop(0, local // LANES, widen, 0)

    def move(c, carry):
        move_rows(pos_ref, c * LANES, src, c * LANES, dst, LANES)
        return carry

    lax.fori_loop(0, local // LANES, move, 0)
    line = lax.broadcasted_iota(jnp.int32, (TAIL, x_ref.shape[1]), 0)

    def narrow(d, carry):
        first = pl.multiple_of(d * per, 8)
        out_ref[d, :per, :LANES] = dst[pl.ds(first, per), :].astype(BF16)
        out_ref[d, :per, LANES:] = dst[pl.ds(first + local, per), :].astype(BF16)
        high = tail_ref[pl.ds(d, 1), :]
        low = tail_ref[pl.ds(d + devices, 1), :]
        out_ref[d, per:, :] = jnp.where(line == 0, high, jnp.where(line == 1, low, 0.0)).astype(BF16)
        return carry

    lax.fori_loop(0, devices, narrow, 0)


def scatter_rows(positions, rows, tail, per):
    local, width = rows.shape
    devices = tail.shape[0] // 2
    return pl.pallas_call(
        functools.partial(scatter_kernel, per=per),
        in_specs=[
            pl.BlockSpec(memory_space=pltpu.SMEM),
            pl.BlockSpec(memory_space=pltpu.VMEM),
            pl.BlockSpec(memory_space=pltpu.VMEM),
        ],
        out_shape=jax.ShapeDtypeStruct((devices, per + TAIL, width), BF16),
        scratch_shapes=[pltpu.VMEM((2 * local, LANES), F32)] * 2,
        compiler_params=params(),
        name="scatter_rows",
    )(positions, rows, tail)


def slice_weights(standard, feeder_t, logit_t, sharp_ref, offset_ref, logit_ref, weight_ref, total_ref):
    heads = sharp_ref.shape[0]
    slices = offset_ref.shape[1]
    middle = lax.dot_general(feeder_t[...], standard, NT, preferred_element_type=F32).astype(BF16)
    logit_ref[...] = jnp.dot(logit_t[...], middle, preferred_element_type=F32)
    sharp = sharp_ref[...]

    def column(c, carry):
        lanes = pl.ds(pl.multiple_of(c * LANES, LANES), LANES)
        top = None
        for m in range(slices):
            value = (logit_ref[m * heads : (m + 1) * heads, lanes] + offset_ref[0, m]) * sharp
            top = value if top is None else jnp.maximum(top, value)
        total = None
        for m in range(slices):
            value = (logit_ref[m * heads : (m + 1) * heads, lanes] + offset_ref[0, m]) * sharp
            value = jnp.exp2(value - top)
            logit_ref[m * heads : (m + 1) * heads, lanes] = value
            total = value if total is None else total + value
        scale = 1.0 / total
        for m in range(slices):
            value = logit_ref[m * heads : (m + 1) * heads, lanes] * scale
            weight_ref[m * heads : (m + 1) * heads, lanes] = value.astype(BF16)
            if total_ref is not None:
                total_ref[m * heads : (m + 1) * heads, :] += value
        return carry

    lax.fori_loop(0, weight_ref.shape[1] // LANES, column, 0)


def head_mask(rows, width, heads):
    row_head = lax.broadcasted_iota(jnp.int32, (rows, width), 0) % heads
    return row_head == lax.broadcasted_iota(jnp.int32, (rows, width), 1) // (width // heads)


def sums_kernel(
    x_ref, gain, bias, attribute, feeder_t, partition_t, sharp_ref, offset_ref,
    packed_ref, logit_t, logit_ref, weight_ref, total_ref, numer_ref,
):
    step = pl.program_id(0)
    heads = sharp_ref.shape[0]
    rows, width = numer_ref.shape
    slices = rows // heads

    @pl.when(step == 0)
    def _():
        total_ref[...] = jnp.zeros_like(total_ref)
        numer_ref[...] = jnp.zeros_like(numer_ref)
        wide = jnp.broadcast_to(partition_t[...].astype(F32)[:, None, :], (slices, heads, width))
        logit_t[...] = jnp.where(
            head_mask(rows, width, heads), wide.reshape(rows, width), 0.0
        ).astype(BF16)

    standard = norm_rows(x_ref[...].astype(F32), gain[...], bias[...]).astype(BF16)
    features = jnp.dot(standard, attribute[...], preferred_element_type=F32).astype(BF16)
    slice_weights(
        standard, feeder_t, logit_t, sharp_ref, offset_ref, logit_ref, weight_ref, total_ref
    )
    numer_ref[...] += jnp.dot(weight_ref[...], features, preferred_element_type=F32)

    @pl.when(step == pl.num_programs(0) - 1)
    def _():
        own = jnp.where(head_mask(rows, width, heads), numer_ref[...], 0.0)
        packed_ref[:, :width] = jnp.sum(own.reshape(slices, heads, width), axis=1)
        sums = jnp.sum(total_ref[...], axis=1, keepdims=True)
        lane = lax.broadcasted_iota(jnp.int32, (rows, LANES), 1)
        row_head = lax.broadcasted_iota(jnp.int32, (rows, LANES), 0) % heads
        own = jnp.where(row_head == lane, sums, 0.0)
        packed_ref[:, width:] = jnp.sum(own.reshape(slices, heads, LANES), axis=1)


def local_sums(x, gain, bias, attribute, feeder_t, partition_t, sharp, offset, block):
    local, width = x.shape
    heads = sharp.shape[0]
    slices = partition_t.shape[0]
    rows = slices * heads
    return pl.pallas_call(
        sums_kernel,
        grid=(local // block,),
        in_specs=[
            pl.BlockSpec((block, width), lambda i: (i, 0)),
            whole(gain.shape), whole(bias.shape), whole(attribute.shape), whole(feeder_t.shape),
            whole(partition_t.shape), whole(sharp.shape),
            pl.BlockSpec(memory_space=pltpu.SMEM),
        ],
        out_specs=(whole((slices, width + LANES)), whole((rows, width))),
        out_shape=(
            jax.ShapeDtypeStruct((slices, width + LANES), F32),
            jax.ShapeDtypeStruct((rows, width), BF16),
        ),
        scratch_shapes=[
            pltpu.VMEM((rows, block), F32),
            pltpu.VMEM((rows, block), BF16),
            pltpu.VMEM((rows, LANES), F32),
            pltpu.VMEM((rows, width), F32),
        ],
        compiler_params=params(),
        cost_estimate=pl.CostEstimate(flops=5_000_000_000, bytes_accessed=4_000_000, transcendentals=3_000_000),
        name="local_sums",
    )(x, gain, bias, attribute, feeder_t, partition_t, sharp, offset)


def attention_kernel(packed_ref, question, lookup, content, mix_t, *, heads):
    highest = lax.Precision.HIGHEST
    slices = packed_ref.shape[0]
    width = packed_ref.shape[1] - LANES
    feature = width // heads
    rows = slices * heads
    spread = (
        lax.broadcasted_iota(jnp.int32, (LANES, width), 0)
        == lax.broadcasted_iota(jnp.int32, (LANES, width), 1) // feature
    ).astype(F32)
    totals = jnp.dot(packed_ref[:, width:], spread, precision=highest, preferred_element_type=F32)
    token = packed_ref[:, :width] / (totals + 1e-05)
    query = jnp.dot(token, question[...], precision=highest, preferred_element_type=F32)
    key = jnp.dot(token, lookup[...], precision=highest, preferred_element_type=F32)
    value = jnp.dot(token, content[...], precision=highest, preferred_element_type=F32)
    mask = head_mask(rows, width, heads)
    query = jnp.broadcast_to(query[:, None, :], (slices, heads, width)).reshape(rows, width)
    query = jnp.where(mask, query, 0.0)
    scores = lax.dot_general(query, key, NT, precision=highest, preferred_element_type=F32)
    scores = scores * (1.0 / math.sqrt(feature))
    scores = jnp.exp(scores - jnp.max(scores, axis=-1, keepdims=True))
    attention = scores / jnp.sum(scores, axis=-1, keepdims=True)
    mixed = jnp.dot(attention, value, precision=highest, preferred_element_type=F32)
    mix_t[...] = jnp.where(mask, mixed, 0.0).T.astype(BF16)


def slice_attention(packed, question, lookup, content, heads):
    slices = packed.shape[0]
    width = packed.shape[1] - LANES
    return pl.pallas_call(
        functools.partial(attention_kernel, heads=heads),
        out_shape=jax.ShapeDtypeStruct((width, slices * heads), BF16),
        compiler_params=params(),
        name="slice_attention",
    )(packed, question, lookup, content)


def finish_kernel(
    pos_ref, x_ref, gain, bias, feeder_t, logit_t, sharp_ref, offset_ref, mix_t, emitted, emitted_offset,
    gain2, bias2, entry, entry_offset, leave, leave_offset,
    out_ref, logit_ref, weight_ref, res, dst, *, per,
):
    step = pl.program_id(0)
    sources = x_ref.shape[0]
    x = jnp.concatenate([x_ref[s, :per, :] for s in range(sources)], axis=0).astype(F32)
    standard = norm_rows(x, gain[...], bias[...]).astype(BF16)
    slice_weights(standard, feeder_t, logit_t, sharp_ref, offset_ref, logit_ref, weight_ref, None)
    blended_t = jnp.dot(mix_t[...], weight_ref[...], preferred_element_type=F32)
    blended = blended_t.T.astype(BF16)
    hidden = x + jnp.dot(blended, emitted[...], preferred_element_type=F32) + emitted_offset[...]
    normed = norm_rows(hidden, gain2[...], bias2[...]).astype(BF16)
    inner = jnp.dot(normed, entry[...], preferred_element_type=F32) + entry_offset[...]
    active = (inner * (1.0 + lax.erf(inner * math.sqrt(0.5)))).astype(BF16)
    result = hidden + jnp.dot(active, leave[...], preferred_element_type=F32) + leave_offset[...]
    block = sources * per
    local = out_ref.shape[0]
    res[:block, :] = result[:, :LANES]
    res[block:, :] = result[:, LANES:]

    def move(c, carry):
        move_rows(pos_ref, step * block + c * LANES, res, c * LANES, dst, LANES)
        return carry

    lax.fori_loop(0, block // LANES, move, 0)

    @pl.when(step == pl.num_programs(0) - 1)
    def _():
        def narrow(c, carry):
            first = pl.multiple_of(c * LANES, LANES)
            out_ref[pl.ds(first, LANES), :LANES] = dst[pl.ds(first, LANES), :].astype(BF16)
            out_ref[pl.ds(first, LANES), LANES:] = dst[pl.ds(first + local, LANES), :].astype(BF16)
            return carry

        lax.fori_loop(0, local // LANES, narrow, 0)


def finish_rows(positions, arrived, gain, bias, feeder_t, logit_t, sharp, offset, mix_t, rest, per, sources):
    devices, stride, width = arrived.shape
    local = devices * per
    rows = logit_t.shape[0]
    block = sources * per
    weights = (gain, bias, feeder_t, logit_t, sharp)
    return pl.pallas_call(
        functools.partial(finish_kernel, per=per),
        grid=(devices // sources,),
        in_specs=[
            pl.BlockSpec(memory_space=pltpu.SMEM),
            pl.BlockSpec((sources, stride, width), lambda i: (i, 0, 0)),
            *[whole(w.shape) for w in weights],
            pl.BlockSpec(memory_space=pltpu.SMEM),
            whole(mix_t.shape),
            *[whole(w.shape) for w in rest],
        ],
        out_specs=whole((local, width)),
        out_shape=jax.ShapeDtypeStruct((local, width), BF16),
        scratch_shapes=[
            pltpu.VMEM((rows, block), F32),
            pltpu.VMEM((rows, block), BF16),
            pltpu.VMEM((2 * block, LANES), F32),
            pltpu.VMEM((2 * local, LANES), F32),
        ],
        compiler_params=params(),
        name="finish_rows",
    )(positions, arrived, *weights, offset, mix_t, *rest)


def sum_devices(value, devices):
    step = 1
    while step < devices:
        value = value + lax.ppermute(
            value, ("head", "pts"), [(i, i ^ step) for i in range(devices)]
        )
        step *= 2
    return value


def body(
    layer_inputs_trainorder,
    inference_placement,
    initial_layernorm_gain,
    initial_layernorm_offset,
    attribute_projection,
    assignment_feeder_projection,
    partition_projection,
    partition_offset,
    softmax_sharpness,
    partition_question_map,
    partition_lookup_map,
    partition_content_map,
    emitted_projection,
    emitted_offset,
    latter_layernorm_gain,
    latter_layernorm_offset,
    perceptron_entry_map,
    perceptron_entry_offset,
    perceptron_exit_map,
    perceptron_exit_offset,
):
    groups = lax.axis_size("head")
    shards = lax.axis_size("pts")
    devices = groups * shards
    local, width = layer_inputs_trainorder.shape
    feature, slices = partition_projection.shape
    heads = width // feature
    per = local // devices
    block = 768 if local % 768 == 0 else LANES
    sources = max(1, block // per)

    own = softmax_sharpness.shape[0]
    place = lax.axis_index("head")
    sharpness = jnp.zeros((groups, own), F32)
    sharpness = lax.dynamic_update_slice(sharpness, softmax_sharpness[None], (place, 0))
    step = 1
    while step < groups:
        sharpness = sharpness + lax.ppermute(
            sharpness, "head", [(i, i ^ step) for i in range(groups)]
        )
        step *= 2
    sharp = jnp.broadcast_to((LOG2E / sharpness.reshape(heads))[:, None], (heads, LANES))

    positions, tail = rank_rows(inference_placement, local, width, groups, shards)
    ordered = scatter_rows(positions.reshape(local), layer_inputs_trainorder, tail, per)
    sharp, ordered = lax.optimization_barrier((sharp, ordered))
    arrived = lax.all_to_all(ordered, ("head", "pts"), split_axis=0, concat_axis=0, tiled=True)
    codes = arrived[:, per : per + 2, :per].astype(F32)
    arrived_at = (codes[:, 0] * LANES + codes[:, 1]).astype(jnp.int32).reshape(local)

    gain = initial_layernorm_gain[None]
    bias = initial_layernorm_offset[None]
    feeder_t = assignment_feeder_projection.T
    partition_t = jnp.tile(partition_projection.T, (1, heads))
    offset = partition_offset[None]
    packed, logit_t = local_sums(
        layer_inputs_trainorder, gain, bias, attribute_projection, feeder_t, partition_t, sharp, offset, block
    )
    packed = sum_devices(packed, devices)
    same = jnp.eye(heads, dtype=F32)
    per_head = [
        jnp.kron(same, w)
        for w in (partition_question_map, partition_lookup_map, partition_content_map)
    ]
    mix_t = slice_attention(packed, *per_head, heads)
    rest = (
        emitted_projection, emitted_offset[None], latter_layernorm_gain[None], latter_layernorm_offset[None],
        perceptron_entry_map, perceptron_entry_offset[None],
        perceptron_exit_map * 0.5, perceptron_exit_offset[None],
    )
    served = finish_rows(
        arrived_at, arrived, gain, bias, feeder_t, logit_t, sharp, offset, mix_t, rest, per, sources
    )
    return served[None]


def solution(mesh):
    rows = P(("head", "pts"))
    placed = (P(("head", "pts"), None), rows, *[P()] * 6, P("head"), *[P()] * 11)
    return jax.shard_map(
        body, mesh=mesh, in_specs=placed, out_specs=P("pts", "head", None), check_vma=False
    )
```

```python
import functools
import math

import jax
import jax.numpy as jnp
from jax import lax
from jax.experimental import pallas as pl
from jax.experimental.pallas import tpu as pltpu
from jax.sharding import PartitionSpec as P

F32 = jnp.float32
BF16 = jnp.bfloat16
LANES = 128
TAIL = 8
EPS_NORM = 1e-05
LOG2E = math.log2(math.e)
NT = (((1,), (1,)), ((), ()))
TN = (((0,), (0,)), ((), ()))
VMEM = 56 * 1024 * 1024


def whole(shape):
    return pl.BlockSpec(shape, lambda *_: (0,) * len(shape))


def params():
    return pltpu.CompilerParams(vmem_limit_bytes=VMEM)


def floor_div(value, divisor):
    return jnp.floor((value + 0.5) * (1.0 / divisor))


def norm_rows(row_block, gain, bias):
    mean = jnp.mean(row_block, axis=-1, keepdims=True)
    centred = row_block - mean
    spread = jnp.mean(centred * centred, axis=-1, keepdims=True)
    return centred * lax.rsqrt(spread + EPS_NORM) * gain + bias


def rank_kernel(place_ref, pos_ref, tail_ref, hot_ref, count_ref, key_ref, *, local, groups, shards, per):
    devices = groups * shards
    chunks = place_ref.shape[0]
    placement = place_ref[...].astype(F32)
    block = floor_div(placement, local)
    within = placement - block * local
    outer = floor_div(block, groups)
    target = (block - outer * groups) * shards + outer
    high = floor_div(within, LANES)
    low = within - high * LANES
    ids = lax.broadcasted_iota(jnp.int32, (devices, LANES), 0).astype(F32)
    for c in range(chunks):
        hot = (ids == target[c : c + 1, :]).astype(F32)
        hot_ref[:, c * LANES : (c + 1) * LANES] = hot.astype(BF16)
    before = lax.broadcasted_iota(jnp.int32, (LANES, LANES), 0) < lax.broadcasted_iota(
        jnp.int32, (LANES, LANES), 1
    )
    prefix = jnp.concatenate(
        [before.astype(F32), jnp.ones((LANES, LANES), F32)], axis=1
    ).astype(BF16)
    for c in range(chunks):
        count_ref[c * devices : (c + 1) * devices, :] = jnp.dot(
            hot_ref[:, c * LANES : (c + 1) * LANES], prefix, preferred_element_type=F32
        )
    carry = jnp.zeros((devices, LANES), F32)
    padded = key_ref.shape[0] // 2
    slots = lax.broadcasted_iota(jnp.int32, (padded, LANES), 0).astype(F32)
    for c in range(chunks):
        counts = count_ref[c * devices : (c + 1) * devices, :]
        hot = hot_ref[:, c * LANES : (c + 1) * LANES].astype(F32)
        rank = jnp.sum(hot * (counts[:, :LANES] + carry), axis=0, keepdims=True)
        carry = carry + counts[:, LANES:]
        pos_ref[c : c + 1, :] = (target[c : c + 1, :] * per + rank).astype(jnp.int32)
        chosen = slots == rank
        key_ref[:padded, c * LANES : (c + 1) * LANES] = jnp.where(
            chosen, high[c : c + 1, :], 0.0
        ).astype(BF16)
        key_ref[padded:, c * LANES : (c + 1) * LANES] = jnp.where(
            chosen, low[c : c + 1, :], 0.0
        ).astype(BF16)
    codes = lax.dot_general(hot_ref[...], key_ref[...], NT, preferred_element_type=F32)
    tail_ref[...] = jnp.zeros_like(tail_ref)
    tail_ref[:devices, :padded] = codes[:, :padded]
    tail_ref[devices:, :padded] = codes[:, padded:]


def rank_rows(placement, local, width, groups, shards):
    devices = groups * shards
    per = local // devices
    padded = -(-per // LANES) * LANES
    chunks = local // LANES
    return pl.pallas_call(
        functools.partial(rank_kernel, local=local, groups=groups, shards=shards, per=per),
        out_shape=(
            jax.ShapeDtypeStruct((chunks, LANES), jnp.int32),
            jax.ShapeDtypeStruct((2 * devices, width), F32),
        ),
        scratch_shapes=[
            pltpu.VMEM((devices, local), BF16),
            pltpu.VMEM((chunks * devices, 2 * LANES), F32),
            pltpu.VMEM((2 * padded, local), BF16),
        ],
        compiler_params=params(),
        name="rank_rows",
    )(placement.reshape(chunks, LANES))


def move_rows(slots_ref, first, source_ref, start, target_ref, count):
    source_half = source_ref.shape[0] // 2
    target_half = target_ref.shape[0] // 2
    for j in range(count):
        slot = slots_ref[first + j]
        target_ref[pl.ds(slot, 1), :] = source_ref[pl.ds(start + j, 1), :]
        target_ref[pl.ds(slot + target_half, 1), :] = source_ref[pl.ds(start + (source_half + j), 1), :]


def scatter_kernel(pos_ref, x_ref, tail_ref, one_ref, two_ref, src, dst, *, first):
    local = x_ref.shape[0]
    devices = tail_ref.shape[0] // 2
    second = two_ref.shape[1]
    per = first + second

    def widen(c, carry):
        row = pl.multiple_of(c * LANES, LANES)
        src[pl.ds(row, LANES), :] = x_ref[pl.ds(row, LANES), :LANES].astype(F32)
        src[pl.ds(row + local, LANES), :] = x_ref[pl.ds(row, LANES), LANES:].astype(F32)
        return carry

    lax.fori_loop(0, local // LANES, widen, 0)

    def move(c, carry):
        move_rows(pos_ref, c * LANES, src, c * LANES, dst, LANES)
        return carry

    lax.fori_loop(0, local // LANES, move, 0)
    line = lax.broadcasted_iota(jnp.int32, (TAIL, x_ref.shape[1]), 0)

    def narrow(d, carry):
        row = pl.multiple_of(d * per, 8)
        one_ref[d, :first, :LANES] = dst[pl.ds(row, first), :].astype(BF16)
        one_ref[d, :first, LANES:] = dst[pl.ds(row + local, first), :].astype(BF16)
        two_ref[d, :, :LANES] = dst[pl.ds(row + first, second), :].astype(BF16)
        two_ref[d, :, LANES:] = dst[pl.ds(row + (first + local), second), :].astype(BF16)
        high = tail_ref[pl.ds(d, 1), :]
        low = tail_ref[pl.ds(d + devices, 1), :]
        one_ref[d, first:, :] = jnp.where(line == 0, high, jnp.where(line == 1, low, 0.0)).astype(BF16)
        return carry

    lax.fori_loop(0, devices, narrow, 0)


def scatter_rows(positions, rows, tail, first, second):
    local, width = rows.shape
    devices = tail.shape[0] // 2
    return pl.pallas_call(
        functools.partial(scatter_kernel, first=first),
        in_specs=[
            pl.BlockSpec(memory_space=pltpu.SMEM),
            pl.BlockSpec(memory_space=pltpu.VMEM),
            pl.BlockSpec(memory_space=pltpu.VMEM),
        ],
        out_shape=(
            jax.ShapeDtypeStruct((devices, first + TAIL, width), BF16),
            jax.ShapeDtypeStruct((devices, second, width), BF16),
        ),
        scratch_shapes=[pltpu.VMEM((2 * local, LANES), F32)] * 2,
        compiler_params=params(),
        name="scatter_rows",
    )(positions, rows, tail)


def slice_weights(standard, feeder_t, logit_t, sharp_ref, offset_ref, logit_ref, weight_ref, total_ref):
    heads = sharp_ref.shape[0]
    slices = offset_ref.shape[1]
    middle = lax.dot_general(feeder_t[...], standard, NT, preferred_element_type=F32).astype(BF16)
    logit_ref[...] = jnp.dot(logit_t[...], middle, preferred_element_type=F32)
    sharp = jnp.broadcast_to(sharp_ref[...], (heads, LANES))
    for start in range(0, weight_ref.shape[1], LANES):
        lanes = pl.ds(start, LANES)
        top = None
        for m in range(slices):
            value = (logit_ref[m * heads : (m + 1) * heads, lanes] + offset_ref[0, m]) * sharp
            top = value if top is None else jnp.maximum(top, value)
        total = None
        for m in range(slices):
            value = (logit_ref[m * heads : (m + 1) * heads, lanes] + offset_ref[0, m]) * sharp
            value = jnp.exp2(value - top)
            logit_ref[m * heads : (m + 1) * heads, lanes] = value
            total = value if total is None else total + value
        scale = 1.0 / total
        for m in range(slices):
            value = logit_ref[m * heads : (m + 1) * heads, lanes] * scale
            weight_ref[m * heads : (m + 1) * heads, lanes] = value.astype(BF16)
            if total_ref is not None:
                total_ref[m * heads : (m + 1) * heads, :] += value


def head_mask(rows, width, heads):
    row_head = lax.broadcasted_iota(jnp.int32, (rows, width), 0) % heads
    return row_head == lax.broadcasted_iota(jnp.int32, (rows, width), 1) // (width // heads)


def sums_kernel(
    x_ref, gain, bias, attribute, feeder_t, partition_t, sharp_ref, offset_ref,
    packed_ref, logit_t, logit_ref, weight_ref, total_ref, numer_ref,
):
    step = pl.program_id(0)
    heads = sharp_ref.shape[0]
    rows, width = numer_ref.shape
    slices = rows // heads

    @pl.when(step == 0)
    def _():
        total_ref[...] = jnp.zeros_like(total_ref)
        numer_ref[...] = jnp.zeros_like(numer_ref)
        wide = jnp.broadcast_to(partition_t[...].astype(F32)[:, None, :], (slices, heads, width))
        logit_t[...] = jnp.where(
            head_mask(rows, width, heads), wide.reshape(rows, width), 0.0
        ).astype(BF16)

    standard = norm_rows(x_ref[...].astype(F32), gain[...], bias[...]).astype(BF16)
    features = jnp.dot(standard, attribute[...], preferred_element_type=F32).astype(BF16)
    slice_weights(
        standard, feeder_t, logit_t, sharp_ref, offset_ref, logit_ref, weight_ref, total_ref
    )
    numer_ref[...] += jnp.dot(weight_ref[...], features, preferred_element_type=F32)

    @pl.when(step == pl.num_programs(0) - 1)
    def _():
        own = jnp.where(head_mask(rows, width, heads), numer_ref[...], 0.0)
        packed_ref[:, :width] = jnp.sum(own.reshape(slices, heads, width), axis=1)
        sums = jnp.sum(total_ref[...], axis=1, keepdims=True)
        lane = lax.broadcasted_iota(jnp.int32, (rows, LANES), 1)
        row_head = lax.broadcasted_iota(jnp.int32, (rows, LANES), 0) % heads
        own = jnp.where(row_head == lane, sums, 0.0)
        packed_ref[:, width:] = jnp.sum(own.reshape(slices, heads, LANES), axis=1)


def local_sums(x, gain, bias, attribute, feeder_t, partition_t, sharp, offset, block):
    local, width = x.shape
    heads = sharp.shape[0]
    slices = partition_t.shape[0]
    rows = slices * heads
    return pl.pallas_call(
        sums_kernel,
        grid=(local // block,),
        in_specs=[
            pl.BlockSpec((block, width), lambda i: (i, 0)),
            whole(gain.shape), whole(bias.shape), whole(attribute.shape), whole(feeder_t.shape),
            whole(partition_t.shape), whole(sharp.shape),
            pl.BlockSpec(memory_space=pltpu.SMEM),
        ],
        out_specs=(whole((slices, width + LANES)), whole((rows, width))),
        out_shape=(
            jax.ShapeDtypeStruct((slices, width + LANES), F32),
            jax.ShapeDtypeStruct((rows, width), BF16),
        ),
        scratch_shapes=[
            pltpu.VMEM((rows, block), F32),
            pltpu.VMEM((rows, block), BF16),
            pltpu.VMEM((rows, LANES), F32),
            pltpu.VMEM((rows, width), F32),
        ],
        compiler_params=params(),
        cost_estimate=pl.CostEstimate(flops=5_000_000_000, bytes_accessed=4_000_000, transcendentals=3_000_000),
        name="local_sums",
    )(x, gain, bias, attribute, feeder_t, partition_t, sharp, offset)


def attention_kernel(packed_ref, question, lookup, content, mix_t, *, heads):
    highest = lax.Precision.HIGHEST
    slices = packed_ref.shape[0]
    width = packed_ref.shape[1] - LANES
    feature = width // heads
    rows = slices * heads
    spread = (
        lax.broadcasted_iota(jnp.int32, (LANES, width), 0)
        == lax.broadcasted_iota(jnp.int32, (LANES, width), 1) // feature
    ).astype(F32)
    totals = jnp.dot(packed_ref[:, width:], spread, precision=highest, preferred_element_type=F32)
    token = packed_ref[:, :width] / (totals + 1e-05)
    own = (
        lax.broadcasted_iota(jnp.int32, (width, width), 0) // feature
        == lax.broadcasted_iota(jnp.int32, (width, width), 1) // feature
    )

    def per_head(weight):
        tiled = jnp.broadcast_to(weight[...][None], (heads, feature, width)).reshape(width, width)
        return jnp.dot(token, jnp.where(own, tiled, 0.0), precision=highest, preferred_element_type=F32)

    query = per_head(question)
    key = per_head(lookup)
    value = per_head(content)
    mask = head_mask(rows, width, heads)
    query = jnp.broadcast_to(query[:, None, :], (slices, heads, width)).reshape(rows, width)
    query = jnp.where(mask, query, 0.0)
    scores = lax.dot_general(query, key, NT, precision=highest, preferred_element_type=F32)
    scores = scores * (1.0 / math.sqrt(feature))
    scores = jnp.exp(scores - jnp.max(scores, axis=-1, keepdims=True))
    attention = scores / jnp.sum(scores, axis=-1, keepdims=True)
    mixed = jnp.dot(attention, value, precision=highest, preferred_element_type=F32)
    mix_t[...] = jnp.where(mask, mixed, 0.0).T.astype(BF16)


def slice_attention(packed, question, lookup, content, heads):
    slices = packed.shape[0]
    width = packed.shape[1] - LANES
    return pl.pallas_call(
        functools.partial(attention_kernel, heads=heads),
        out_shape=jax.ShapeDtypeStruct((width, slices * heads), BF16),
        compiler_params=params(),
        name="slice_attention",
    )(packed, question, lookup, content)


def finish_kernel(
    pos_ref, x_ref, gain, bias, feeder_t, logit_t, sharp_ref, offset_ref, mix_t, emitted, emitted_offset,
    gain2, bias2, entry, entry_offset, leave, leave_offset, *refs, per, last,
):
    if last:
        before, out_ref, logit_ref, weight_ref, res, dst, stage, sem = refs
    else:
        out_ref, logit_ref, weight_ref, res, dst, sem = refs
    step = pl.program_id(0)
    sources = x_ref.shape[0]
    block = sources * per
    local = dst.shape[0] // 2

    def carry_over(other, inward):
        for k in range(2):
            mine = dst.at[pl.ds(k * local, local)]
            far = other.at[pl.ds(k * local, local)]
            yield pltpu.make_async_copy(*((far, mine) if inward else (mine, far)), sem.at[k])

    if last:

        @pl.when(step == 0)
        def _():
            for copy in carry_over(before, True):
                copy.start()

    x = jnp.concatenate([x_ref[s, :per, :] for s in range(sources)], axis=0).astype(F32)
    standard = norm_rows(x, gain[...], bias[...]).astype(BF16)
    slice_weights(standard, feeder_t, logit_t, sharp_ref, offset_ref, logit_ref, weight_ref, None)
    blended_t = jnp.dot(mix_t[...], weight_ref[...], preferred_element_type=F32)
    blended = blended_t.T.astype(BF16)
    hidden = x + jnp.dot(blended, emitted[...], preferred_element_type=F32) + emitted_offset[...]
    normed = norm_rows(hidden, gain2[...], bias2[...]).astype(BF16)
    inner = jnp.dot(normed, entry[...], preferred_element_type=F32) + entry_offset[...]
    active = (inner * (1.0 + lax.erf(inner * math.sqrt(0.5)))).astype(BF16)
    result = hidden + jnp.dot(active, leave[...], preferred_element_type=F32) + leave_offset[...]
    res[:block, :] = result[:, :LANES]
    res[block:, :] = result[:, LANES:]

    if last:

        @pl.when(step == 0)
        def _():
            for copy in carry_over(before, True):
                copy.wait()

    def move(c, carry):
        move_rows(pos_ref, step * block + c * LANES, res, c * LANES, dst, LANES)
        return carry

    lax.fori_loop(0, block // LANES, move, 0)

    @pl.when(step == pl.num_programs(0) - 1)
    def _():
        if not last:
            copies = list(carry_over(out_ref, False))
            for copy in copies:
                copy.start()
            for copy in copies:
                copy.wait()
        else:
            parts = sem.shape[0]
            size = local // parts
            copies = []
            for q in range(parts):

                def narrow(c, carry, q=q):
                    row = pl.multiple_of(q * size + c * LANES, LANES)
                    stage[pl.ds(row, LANES), :LANES] = dst[pl.ds(row, LANES), :].astype(BF16)
                    stage[pl.ds(row, LANES), LANES:] = dst[pl.ds(row + local, LANES), :].astype(BF16)
                    return carry

                lax.fori_loop(0, size // LANES, narrow, 0)
                rows = pl.ds(q * size, size)
                copies.append(pltpu.make_async_copy(stage.at[rows], out_ref.at[rows], sem.at[q]))
                copies[-1].start()
            for copy in copies:
                copy.wait()


def finish_rows(positions, arrived, weights, offset, mix_t, rest, before, local, per, sources):
    devices, stride, width = arrived.shape
    rows = mix_t.shape[1]
    block = sources * per
    last = before is not None
    shape = (local, width) if last else (2 * local, LANES)
    return pl.pallas_call(
        functools.partial(finish_kernel, per=per, last=last),
        grid=(devices // sources,),
        in_specs=[
            pl.BlockSpec(memory_space=pltpu.SMEM),
            pl.BlockSpec((sources, stride, width), lambda i: (i, 0, 0)),
            *[whole(w.shape) for w in weights],
            pl.BlockSpec(memory_space=pltpu.SMEM),
            whole(mix_t.shape),
            *[whole(w.shape) for w in rest],
            *([pl.BlockSpec(memory_space=pl.ANY)] if last else []),
        ],
        out_specs=pl.BlockSpec(memory_space=pl.ANY),
        out_shape=jax.ShapeDtypeStruct(shape, BF16 if last else F32),
        scratch_shapes=[
            pltpu.VMEM((rows, block), F32),
            pltpu.VMEM((rows, block), BF16),
            pltpu.VMEM((2 * block, LANES), F32),
            pltpu.VMEM((2 * local, LANES), F32),
            *([pltpu.VMEM((local, width), BF16)] if last else []),
            pltpu.SemaphoreType.DMA((4 if last else 2,)),
        ],
        compiler_params=params(),
        cost_estimate=pl.CostEstimate(
            flops=2_000_000 * devices * per, bytes_accessed=8_000_000, transcendentals=1000 * devices * per
        ),
        name="finish_last" if last else "finish_first",
    )(positions, arrived, *weights, offset, mix_t, *rest, *([before] if last else []))


def sum_devices(value, groups, shards):
    step = 1
    while step < shards:
        value = value + lax.ppermute(value, "pts", [(i, i ^ step) for i in range(shards)])
        step *= 2
    others = [lax.ppermute(value, "head", [(i, i ^ k) for i in range(groups)]) for k in range(1, groups)]
    for other in others:
        value = value + other
    return value


def body(
    layer_inputs_trainorder,
    inference_placement,
    initial_layernorm_gain,
    initial_layernorm_offset,
    attribute_projection,
    assignment_feeder_projection,
    partition_projection,
    partition_offset,
    softmax_sharpness,
    partition_question_map,
    partition_lookup_map,
    partition_content_map,
    emitted_projection,
    emitted_offset,
    latter_layernorm_gain,
    latter_layernorm_offset,
    perceptron_entry_map,
    perceptron_entry_offset,
    perceptron_exit_map,
    perceptron_exit_offset,
):
    groups = lax.axis_size("head")
    shards = lax.axis_size("pts")
    devices = groups * shards
    local, width = layer_inputs_trainorder.shape
    feature, slices = partition_projection.shape
    heads = width // feature
    per = local // devices
    block = 768 if local % 768 == 0 else LANES
    first = per * 2 // 3
    second = per - first
    rows_at_once = 8 * LANES

    mates = [
        lax.ppermute(softmax_sharpness, "head", [(i, i ^ k) for i in range(groups)])
        for k in range(1, groups)
    ]
    positions, tail = rank_rows(inference_placement, local, width, groups, shards)
    one, two = scatter_rows(positions.reshape(local), layer_inputs_trainorder, tail, first, second)
    *mates, one, two = lax.optimization_barrier((*mates, one, two))
    arrived_one = lax.all_to_all(one, ("head", "pts"), split_axis=0, concat_axis=0, tiled=True)

    place = lax.axis_index("head")
    order = jnp.arange(groups)[:, None]
    sharp = jnp.where(order == place, softmax_sharpness[None], 0.0)
    for k, mate in enumerate(mates, 1):
        sharp = jnp.where(order == (place ^ k), mate[None], sharp)
    sharp = (LOG2E / sharp).reshape(heads, 1)
    gain = initial_layernorm_gain[None]
    bias = initial_layernorm_offset[None]
    feeder_t = assignment_feeder_projection.T
    partition_t = jnp.tile(partition_projection.T, (1, heads))
    offset = partition_offset[None]
    packed, logit_t = local_sums(
        layer_inputs_trainorder, gain, bias, attribute_projection, feeder_t, partition_t, sharp, offset, block
    )
    packed = sum_devices(packed, groups, shards)
    packed, arrived_one, two = lax.optimization_barrier((packed, arrived_one, two))
    arrived_two = lax.all_to_all(two, ("head", "pts"), split_axis=0, concat_axis=0, tiled=True)

    codes = arrived_one[:, first : first + 2, :per].astype(F32)
    arrived_at = (codes[:, 0] * LANES + codes[:, 1]).astype(jnp.int32)
    maps = [
        jnp.tile(w, (1, heads))
        for w in (partition_question_map, partition_lookup_map, partition_content_map)
    ]
    mix_t = slice_attention(packed, *maps, heads)
    weights = (gain, bias, feeder_t, logit_t, sharp)
    rest = (
        emitted_projection, emitted_offset[None], latter_layernorm_gain[None], latter_layernorm_offset[None],
        perceptron_entry_map, perceptron_entry_offset[None],
        perceptron_exit_map * 0.5, perceptron_exit_offset[None],
    )
    placed = finish_rows(
        arrived_at[:, :first].reshape(-1), arrived_one, weights, offset, mix_t, rest, None, local, first,
        rows_at_once // first,
    )
    served = finish_rows(
        arrived_at[:, first:].reshape(-1), arrived_two, weights, offset, mix_t, rest, placed, local, second,
        rows_at_once // second,
    )
    return served[None]


def solution(mesh):
    rows = P(("head", "pts"))
    placed = (P(("head", "pts"), None), rows, *[P()] * 6, P("head"), *[P()] * 11)
    return jax.shard_map(
        body, mesh=mesh, in_specs=placed, out_specs=P("pts", "head", None), check_vma=False
    )
```

```python
import functools
import math

import jax
import jax.numpy as jnp
from jax import lax
from jax.experimental import pallas as pl
from jax.experimental.pallas import tpu as pltpu
from jax.sharding import PartitionSpec as P


F32 = jnp.float32
BF16 = jnp.bfloat16
LANES = 128
TAIL = 8
BLOCK = 1024
EPS_NORM = 1e-05
LOG2E = math.log2(math.e)
NT = (((1,), (1,)), ((), ()))
TN = (((0,), (0,)), ((), ()))
NN = (((1,), (0,)), ((), ()))
VMEM = 56 * 1024 * 1024


def whole(shape):
    return pl.BlockSpec(shape, lambda *_: (0,) * len(shape))


def params():
    return pltpu.CompilerParams(vmem_limit_bytes=VMEM)


def floor_div(value, divisor):
    return jnp.floor((value + 0.5) * (1.0 / divisor))


def norm_rows(row_block, gain, bias):
    mean = jnp.mean(row_block, axis=-1, keepdims=True)
    centred = row_block - mean
    spread = jnp.mean(centred * centred, axis=-1, keepdims=True)
    return centred * lax.rsqrt(spread + EPS_NORM) * gain + bias


def rank_kernel(place_ref, list_ref, tail_ref, hot_ref, count_ref, key_ref, *, local, groups, shards):
    devices = groups * shards
    chunks = place_ref.shape[0]
    padded = list_ref.shape[1]
    placement = place_ref[...].astype(F32)
    block = floor_div(placement, local)
    within = placement - block * local
    outer = floor_div(block, groups)
    target = (block - outer * groups) * shards + outer
    high = floor_div(within, LANES)
    low = within - high * LANES
    ids = lax.broadcasted_iota(jnp.int32, (devices, LANES), 0).astype(F32)
    for c in range(chunks):
        hot = (ids == target[c : c + 1, :]).astype(F32)
        hot_ref[:, c * LANES : (c + 1) * LANES] = hot.astype(BF16)
    before = lax.broadcasted_iota(jnp.int32, (LANES, LANES), 0) < lax.broadcasted_iota(
        jnp.int32, (LANES, LANES), 1
    )
    prefix = jnp.concatenate(
        [before.astype(F32), jnp.ones((LANES, LANES), F32)], axis=1
    ).astype(BF16)
    for c in range(chunks):
        count_ref[c * devices : (c + 1) * devices, :] = jnp.dot(
            hot_ref[:, c * LANES : (c + 1) * LANES], prefix, preferred_element_type=F32
        )
    carry = jnp.zeros((devices, LANES), F32)
    slots = lax.broadcasted_iota(jnp.int32, (padded, LANES), 0).astype(F32)
    lane = lax.broadcasted_iota(jnp.int32, (1, LANES), 1).astype(F32)
    for c in range(chunks):
        counts = count_ref[c * devices : (c + 1) * devices, :]
        hot = hot_ref[:, c * LANES : (c + 1) * LANES].astype(F32)
        rank = jnp.sum(hot * (counts[:, :LANES] + carry), axis=0, keepdims=True)
        carry = carry + counts[:, LANES:]
        chosen = slots == rank
        values = (high[c : c + 1, :], low[c : c + 1, :], float(c), lane)
        for k, value in enumerate(values):
            key_ref[k * padded : (k + 1) * padded, c * LANES : (c + 1) * LANES] = jnp.where(
                chosen, value, 0.0
            ).astype(BF16)
    codes = lax.dot_general(hot_ref[...], key_ref[...], NT, preferred_element_type=F32)
    tail_ref[...] = jnp.zeros_like(tail_ref)
    tail_ref[:devices, :padded] = codes[:, :padded]
    tail_ref[devices:, :padded] = codes[:, padded : 2 * padded]
    source = codes[:, 2 * padded : 3 * padded] * LANES + codes[:, 3 * padded :]
    list_ref[...] = source.astype(jnp.int32)


def rank_rows(placement, local, width, groups, shards):
    devices = groups * shards
    per = local // devices
    padded = -(-per // LANES) * LANES
    chunks = local // LANES
    return pl.pallas_call(
        functools.partial(rank_kernel, local=local, groups=groups, shards=shards),
        out_shape=(
            jax.ShapeDtypeStruct((devices, padded), jnp.int32),
            jax.ShapeDtypeStruct((2 * devices, width), F32),
        ),
        scratch_shapes=[
            pltpu.VMEM((devices, local), BF16),
            pltpu.VMEM((chunks * devices, 2 * LANES), F32),
            pltpu.VMEM((4 * padded, local), BF16),
        ],
        compiler_params=params(),
        name="rank_rows",
    )(placement.reshape(chunks, LANES))


def gather_kernel(list_ref, x_ref, *refs, start, counts, tailed):
    tail_ref = refs[0] if tailed else None
    outs = refs[1 if tailed else 0 : -2]
    src, dst = refs[-2:]
    local, width = x_ref.shape
    devices = list_ref.shape[0]
    total = sum(counts)

    def widen(c, carry):
        row = pl.multiple_of(c * LANES, LANES)
        src[pl.ds(row, LANES), :] = x_ref[pl.ds(row, LANES), :LANES].astype(F32)
        src[pl.ds(row + local, LANES), :] = x_ref[pl.ds(row, LANES), LANES:].astype(F32)
        return carry

    lax.fori_loop(0, local // LANES, widen, 0)
    line = lax.broadcasted_iota(jnp.int32, (TAIL, width), 0)

    def fetch(d, carry):
        for j in range(total):
            row = list_ref[d, start + j]
            dst[j : j + 1, :] = src[pl.ds(row, 1), :]
            dst[total + j : total + j + 1, :] = src[pl.ds(row + local, 1), :]
        done = 0
        for out, count in zip(outs, counts):
            out[d, :count, :LANES] = dst[done : done + count, :].astype(BF16)
            out[d, :count, LANES:] = dst[total + done : total + done + count, :].astype(BF16)
            done += count
        if tailed:
            high = tail_ref[pl.ds(d, 1), :]
            low = tail_ref[pl.ds(d + devices, 1), :]
            codes = jnp.where(line == 0, high, jnp.where(line == 1, low, 0.0))
            outs[0][d, counts[0] :, :] = codes.astype(BF16)
        return carry

    lax.fori_loop(0, devices, fetch, 0)


def gather_rows(lists, rows, tail, start, counts):
    local, width = rows.shape
    devices = lists.shape[0]
    tailed = tail is not None
    vmem = pl.BlockSpec(memory_space=pltpu.VMEM)
    out_shape = [
        jax.ShapeDtypeStruct((devices, n + (TAIL if tailed else 0), width), BF16) for n in counts
    ]
    return pl.pallas_call(
        functools.partial(gather_kernel, start=start, counts=counts, tailed=tailed),
        in_specs=[pl.BlockSpec(memory_space=pltpu.SMEM), vmem, *([vmem] if tailed else [])],
        out_shape=out_shape,
        scratch_shapes=[
            pltpu.VMEM((2 * local, LANES), F32),
            pltpu.VMEM((2 * sum(counts), LANES), F32),
        ],
        compiler_params=params(),
        cost_estimate=pl.CostEstimate(
            flops=2_000_000 * devices * sum(counts), bytes_accessed=6_000_000, transcendentals=0
        ),
        name="gather_first" if tailed else "gather_rest",
    )(lists, rows, *([tail] if tailed else []))


def slice_weights(standard, feeder_t, logit_t, sharp_ref, offset_ref, logit_ref, weight_ref, total_ref):
    heads = sharp_ref.shape[0]
    slices = offset_ref.shape[1]
    middle = lax.dot_general(feeder_t[...], standard, NT, preferred_element_type=F32).astype(BF16)
    logit_ref[...] = jnp.dot(logit_t[...], middle, preferred_element_type=F32)
    sharp = jnp.broadcast_to(sharp_ref[...], (heads, LANES))
    for start in range(0, weight_ref.shape[1], LANES):
        lanes = pl.ds(start, LANES)
        top = None
        for m in range(slices):
            value = (logit_ref[m * heads : (m + 1) * heads, lanes] + offset_ref[0, m]) * sharp
            top = value if top is None else jnp.maximum(top, value)
        total = None
        for m in range(slices):
            value = (logit_ref[m * heads : (m + 1) * heads, lanes] + offset_ref[0, m]) * sharp
            value = jnp.exp2(value - top)
            logit_ref[m * heads : (m + 1) * heads, lanes] = value
            total = value if total is None else total + value
        scale = 1.0 / total
        for m in range(slices):
            value = logit_ref[m * heads : (m + 1) * heads, lanes] * scale
            weight_ref[m * heads : (m + 1) * heads, lanes] = value.astype(BF16)
            if total_ref is not None:
                total_ref[m * heads : (m + 1) * heads, :] += value


def head_mask(rows, width, heads):
    row_head = lax.broadcasted_iota(jnp.int32, (rows, width), 0) % heads
    return row_head == lax.broadcasted_iota(jnp.int32, (rows, width), 1) // (width // heads)


def repeat_heads(value, width, dims):
    feature = value.shape[dims[0][0][0]]
    pick = lax.broadcasted_iota(jnp.int32, (feature, width), 1) % feature == lax.broadcasted_iota(
        jnp.int32, (feature, width), 0
    )
    return lax.dot_general(
        value, pick.astype(F32), dims, precision=lax.Precision.HIGHEST, preferred_element_type=F32
    )


def sums_kernel(
    x_ref, gain, bias, attribute, feeder_t, partition, sharp_ref, offset_ref,
    packed_ref, logit_t, logit_ref, weight_ref, total_ref, numer_ref,
):
    step = pl.program_id(0)
    heads = sharp_ref.shape[0]
    rows, width = numer_ref.shape
    slices = rows // heads

    @pl.when(step == 0)
    def _():
        total_ref[...] = jnp.zeros_like(total_ref)
        numer_ref[...] = jnp.zeros_like(numer_ref)
        wide = repeat_heads(partition[...].astype(F32), width, TN)
        wide = jnp.broadcast_to(wide[:, None, :], (slices, heads, width))
        logit_t[...] = jnp.where(
            head_mask(rows, width, heads), wide.reshape(rows, width), 0.0
        ).astype(BF16)

    standard = norm_rows(x_ref[...].astype(F32), gain[...], bias[...]).astype(BF16)
    features = jnp.dot(standard, attribute[...], preferred_element_type=F32).astype(BF16)
    slice_weights(
        standard, feeder_t, logit_t, sharp_ref, offset_ref, logit_ref, weight_ref, total_ref
    )
    numer_ref[...] += jnp.dot(weight_ref[...], features, preferred_element_type=F32)

    @pl.when(step == pl.num_programs(0) - 1)
    def _():
        own = jnp.where(head_mask(rows, width, heads), numer_ref[...], 0.0)
        packed_ref[:, :width] = jnp.sum(own.reshape(slices, heads, width), axis=1)
        sums = jnp.sum(total_ref[...], axis=1, keepdims=True)
        lane = lax.broadcasted_iota(jnp.int32, (rows, LANES), 1)
        row_head = lax.broadcasted_iota(jnp.int32, (rows, LANES), 0) % heads
        own = jnp.where(row_head == lane, sums, 0.0)
        packed_ref[:, width:] = jnp.sum(own.reshape(slices, heads, LANES), axis=1)


def local_sums(x, gain, bias, attribute, feeder_t, partition, sharp, offset, block):
    local, width = x.shape
    heads = sharp.shape[0]
    slices = partition.shape[1]
    rows = slices * heads
    return pl.pallas_call(
        sums_kernel,
        grid=(local // block,),
        in_specs=[
            pl.BlockSpec((block, width), lambda i: (i, 0)),
            whole(gain.shape), whole(bias.shape), whole(attribute.shape), whole(feeder_t.shape),
            whole(partition.shape), whole(sharp.shape),
            pl.BlockSpec(memory_space=pltpu.SMEM),
        ],
        out_specs=(whole((slices, width + LANES)), whole((rows, width))),
        out_shape=(
            jax.ShapeDtypeStruct((slices, width + LANES), F32),
            jax.ShapeDtypeStruct((rows, width), BF16),
        ),
        scratch_shapes=[
            pltpu.VMEM((rows, block), F32),
            pltpu.VMEM((rows, block), BF16),
            pltpu.VMEM((rows, LANES), F32),
            pltpu.VMEM((rows, width), F32),
        ],
        compiler_params=params(),
        cost_estimate=pl.CostEstimate(flops=5_000_000_000, bytes_accessed=4_000_000, transcendentals=3_000_000),
        name="local_sums",
    )(x, gain, bias, attribute, feeder_t, partition, sharp, offset)


def attention_kernel(packed_ref, question, lookup, content, mix_t, *, heads):
    highest = lax.Precision.HIGHEST
    slices = packed_ref.shape[0]
    width = packed_ref.shape[1] - LANES
    feature = width // heads
    rows = slices * heads
    spread = (
        lax.broadcasted_iota(jnp.int32, (LANES, width), 0)
        == lax.broadcasted_iota(jnp.int32, (LANES, width), 1) // feature
    ).astype(F32)
    totals = jnp.dot(packed_ref[:, width:], spread, precision=highest, preferred_element_type=F32)
    token = packed_ref[:, :width] / (totals + 1e-05)
    own = (
        lax.broadcasted_iota(jnp.int32, (width, width), 0) // feature
        == lax.broadcasted_iota(jnp.int32, (width, width), 1) // feature
    )

    def per_head(weight):
        wide = repeat_heads(weight[...], width, NN)
        tiled = jnp.broadcast_to(wide[None], (heads, feature, width)).reshape(width, width)
        return jnp.dot(token, jnp.where(own, tiled, 0.0), precision=highest, preferred_element_type=F32)

    query = per_head(question)
    key = per_head(lookup)
    value = per_head(content)
    mask = head_mask(rows, width, heads)
    query = jnp.broadcast_to(query[:, None, :], (slices, heads, width)).reshape(rows, width)
    query = jnp.where(mask, query, 0.0)
    scores = lax.dot_general(query, key, NT, precision=highest, preferred_element_type=F32)
    scores = scores * (1.0 / math.sqrt(feature))
    scores = jnp.exp(scores - jnp.max(scores, axis=-1, keepdims=True))
    attention = scores / jnp.sum(scores, axis=-1, keepdims=True)
    mixed = jnp.dot(attention, value, precision=highest, preferred_element_type=F32)
    mix_t[...] = jnp.where(mask, mixed, 0.0).T.astype(BF16)


def slice_attention(packed, question, lookup, content, heads):
    slices = packed.shape[0]
    width = packed.shape[1] - LANES
    return pl.pallas_call(
        functools.partial(attention_kernel, heads=heads),
        out_shape=jax.ShapeDtypeStruct((width, slices * heads), BF16),
        compiler_params=params(),
        name="slice_attention",
    )(packed, question, lookup, content)


def finish_kernel(
    pos_ref, x_ref, gain, bias, feeder_t, logit_t, sharp_ref, offset_ref, mix_t, emitted, emitted_offset,
    gain2, bias2, entry, entry_offset, leave, leave_offset, *refs, start, per, follows, last,
):
    refs = list(refs)
    before = refs.pop(0) if follows else None
    out_ref, logit_ref, weight_ref, res, dst, sem = refs[:6]
    step = pl.program_id(0)
    sources = x_ref.shape[0]
    block = sources * per
    local = dst.shape[0] // 2

    def handover(inward):
        if inward:
            return pltpu.make_async_copy(before, dst, sem.at[0])
        return pltpu.make_async_copy(dst, out_ref, sem.at[0])

    if follows:

        @pl.when(step == 0)
        def _():
            handover(True).start()

    x = jnp.concatenate([x_ref[s, :per, :] for s in range(sources)], axis=0).astype(F32)
    standard = norm_rows(x, gain[...], bias[...]).astype(BF16)
    slice_weights(standard, feeder_t, logit_t, sharp_ref, offset_ref, logit_ref, weight_ref, None)
    blended_t = jnp.dot(mix_t[...], weight_ref[...], preferred_element_type=F32)
    blended = blended_t.T.astype(BF16)
    hidden = x + jnp.dot(blended, emitted[...], preferred_element_type=F32) + emitted_offset[...]
    normed = norm_rows(hidden, gain2[...], bias2[...]).astype(BF16)
    inner = jnp.dot(normed, entry[...], preferred_element_type=F32) + entry_offset[...]
    active = (inner * (1.0 + lax.erf(inner * math.sqrt(0.5)))).astype(BF16)
    leaving = jnp.dot(active, leave[...], preferred_element_type=F32)
    result = hidden + 0.5 * leaving + leave_offset[...]
    res[:block, :] = result[:, :LANES]
    res[block:, :] = result[:, LANES:]
    if follows:

        @pl.when(step == 0)
        def _():
            handover(True).wait()

    together = max(k for k in range(1, sources + 1) if sources % k == 0 and k * per <= LANES)

    def move(g, carry):
        for q in range(together):
            source = g * together + q
            for j in range(per):
                slot = pos_ref[step * sources + source, start + j]
                row = g * (together * per) + (q * per + j)
                dst[pl.ds(slot, 1), :] = res[pl.ds(row, 1), :]
                dst[pl.ds(slot + local, 1), :] = res[pl.ds(row + block, 1), :]
        return carry

    lax.fori_loop(0, sources // together, move, 0)

    @pl.when(step == pl.num_programs(0) - 1)
    def _():
        if not last:
            handover(False).start()
            handover(False).wait()
        else:
            stage = refs[6]
            parts = sem.shape[0]
            size = local // parts
            copies = []
            for q in range(parts):

                def narrow(c, carry, q=q):
                    row = pl.multiple_of(q * size + c * LANES, LANES)
                    stage[pl.ds(row, LANES), :LANES] = dst[pl.ds(row, LANES), :].astype(BF16)
                    stage[pl.ds(row, LANES), LANES:] = dst[pl.ds(row + local, LANES), :].astype(BF16)
                    return carry

                lax.fori_loop(0, size // LANES, narrow, 0)
                rows = pl.ds(q * size, size)
                copies.append(pltpu.make_async_copy(stage.at[rows], out_ref.at[rows], sem.at[q]))
                copies[-1].start()
            for copy in copies:
                copy.wait()


def finish_rows(positions, arrived, weights, offset, mix_t, rest, before, local, start, per, last):
    devices, stride, width = arrived.shape
    rows = mix_t.shape[1]
    sources = max(k for k in range(1, devices + 1) if devices % k == 0 and k * per <= BLOCK)
    block = sources * per
    follows = before is not None
    shape = (local, width) if last else (2 * local, LANES)
    return pl.pallas_call(
        functools.partial(finish_kernel, start=start, per=per, follows=follows, last=last),
        grid=(devices // sources,),
        in_specs=[
            pl.BlockSpec(memory_space=pltpu.SMEM),
            pl.BlockSpec((sources, stride, width), lambda i: (i, 0, 0)),
            *[whole(w.shape) for w in weights],
            pl.BlockSpec(memory_space=pltpu.SMEM),
            whole(mix_t.shape),
            *[whole(w.shape) for w in rest],
            *([pl.BlockSpec(memory_space=pl.ANY)] if follows else []),
        ],
        out_specs=pl.BlockSpec(memory_space=pl.ANY),
        out_shape=jax.ShapeDtypeStruct(shape, BF16 if last else F32),
        scratch_shapes=[
            pltpu.VMEM((rows, block), F32),
            pltpu.VMEM((rows, block), BF16),
            pltpu.VMEM((2 * block, LANES), F32),
            pltpu.VMEM((2 * local, LANES), F32),
            pltpu.SemaphoreType.DMA((4 if last else 1,)),
            *([pltpu.VMEM((local, width), BF16)] if last else []),
        ],
        compiler_params=params(),
        cost_estimate=pl.CostEstimate(
            flops=2_000_000 * devices * per, bytes_accessed=8_000_000, transcendentals=1000 * devices * per
        ),
    )(positions, arrived, *weights, offset, mix_t, *rest, *([before] if follows else []))


def sum_plane(value, shards):
    step = 1
    while step < shards:
        value = value + lax.ppermute(value, "pts", [(i, i ^ step) for i in range(shards)])
        step *= 2
    return value


def sum_head(value, groups):
    others = [lax.ppermute(value, "head", [(i, i ^ k) for i in range(groups)]) for k in range(1, groups)]
    for other in others:
        value = value + other
    return value


def body(
    layer_inputs_trainorder,
    inference_placement,
    initial_layernorm_gain,
    initial_layernorm_offset,
    attribute_projection,
    assignment_feeder_projection,
    partition_projection,
    partition_offset,
    softmax_sharpness,
    partition_question_map,
    partition_lookup_map,
    partition_content_map,
    emitted_projection,
    emitted_offset,
    latter_layernorm_gain,
    latter_layernorm_offset,
    perceptron_entry_map,
    perceptron_entry_offset,
    perceptron_exit_map,
    perceptron_exit_offset,
):
    groups = lax.axis_size("head")
    shards = lax.axis_size("pts")
    devices = groups * shards
    local, width = layer_inputs_trainorder.shape
    feature, _ = partition_projection.shape
    heads = width // feature
    per = local // devices
    block = 768 if local % 768 == 0 else LANES
    parts = (per // 2, per // 3, per - per // 2 - per // 3)
    starts = (0, parts[0], parts[0] + parts[1])

    def exchange(rows):
        return lax.all_to_all(rows, ("head", "pts"), split_axis=0, concat_axis=0, tiled=True)

    mates = [
        lax.ppermute(softmax_sharpness, "head", [(i, i ^ k) for i in range(groups)])
        for k in range(1, groups)
    ]
    lists, tail = rank_rows(inference_placement, local, width, groups, shards)
    (one,) = gather_rows(lists, layer_inputs_trainorder, tail, starts[0], parts[:1])
    *mates, one = lax.optimization_barrier((*mates, one))
    arrived_one = exchange(one)
    two, three = gather_rows(lists, layer_inputs_trainorder, None, starts[1], parts[1:])

    place = lax.axis_index("head")
    order = jnp.arange(groups)[:, None]
    sharp = jnp.where(order == place, softmax_sharpness[None], 0.0)
    for k, mate in enumerate(mates, 1):
        sharp = jnp.where(order == (place ^ k), mate[None], sharp)
    sharp = (LOG2E / sharp).reshape(heads, 1)
    gain = initial_layernorm_gain[None]
    bias = initial_layernorm_offset[None]
    feeder_t = assignment_feeder_projection.T
    offset = partition_offset[None]
    packed, logit_t = local_sums(
        layer_inputs_trainorder, gain, bias, attribute_projection, feeder_t, partition_projection, sharp,
        offset, block,
    )
    packed = sum_plane(packed, shards)
    _, arrived_one, two = lax.optimization_barrier((packed, arrived_one, two))
    arrived_two = exchange(two)
    packed = sum_head(packed, groups)

    codes = lax.optimization_barrier(arrived_one[:, parts[0] :, :])[:, :2, :per].astype(F32)
    arrived_at = (codes[:, 0] * LANES + codes[:, 1]).astype(jnp.int32)
    mix_t = slice_attention(
        packed, partition_question_map, partition_lookup_map, partition_content_map, heads
    )
    weights = (gain, bias, feeder_t, logit_t, sharp)
    rest = (
        emitted_projection, emitted_offset[None], latter_layernorm_gain[None], latter_layernorm_offset[None],
        perceptron_entry_map, perceptron_entry_offset[None],
        perceptron_exit_map, perceptron_exit_offset[None],
    )
    served = finish_rows(
        arrived_at, arrived_one, weights, offset, mix_t, rest, None, local, starts[0], parts[0], False
    )
    served, arrived_two, three = lax.optimization_barrier((served, arrived_two, three))
    arrived_three = exchange(three)
    served = finish_rows(
        arrived_at, arrived_two, weights, offset, mix_t, rest, served, local, starts[1], parts[1], False
    )
    served = finish_rows(
        arrived_at, arrived_three, weights, offset, mix_t, rest, served, local, starts[2], parts[2], True
    )
    return served[None]


def solution(mesh):
    rows = P(("head", "pts"))
    placed = (P(("head", "pts"), None), rows, *[P()] * 6, P("head"), *[P()] * 11)

    return jax.shard_map(body, mesh=mesh, in_specs=placed, out_specs=P("pts", "head", None), check_vma=False)
```

```python
import functools
import math

import jax
import jax.numpy as jnp
from jax import lax
from jax.experimental import pallas as pl
from jax.experimental.pallas import tpu as pltpu
from jax.sharding import PartitionSpec as P


F32 = jnp.float32
BF16 = jnp.bfloat16
LANES = 128
TAIL = 8
BLOCK = 1024
EPS_NORM = 1e-05
LOG2E = math.log2(math.e)
NT = (((1,), (1,)), ((), ()))
TN = (((0,), (0,)), ((), ()))
NN = (((1,), (0,)), ((), ()))
VMEM = 56 * 1024 * 1024


def whole(shape):
    return pl.BlockSpec(shape, lambda *_: (0,) * len(shape))


def params():
    return pltpu.CompilerParams(vmem_limit_bytes=VMEM)


def floor_div(value, divisor):
    return jnp.floor((value + 0.5) * (1.0 / divisor))


def norm_rows(row_block, gain, bias):
    mean = jnp.mean(row_block, axis=-1, keepdims=True)
    centred = row_block - mean
    spread = jnp.mean(centred * centred, axis=-1, keepdims=True)
    return centred * lax.rsqrt(spread + EPS_NORM) * gain + bias


def narrow_rows(source, first, other, count):
    low = source[first : first + count, :].astype(BF16)
    return low, source[other : other + count, :].astype(BF16)


def fetch_rows(lists, start, count, src, dst, stage, out, sem, group):
    local = src.shape[0] // 2
    devices = lists.shape[0]
    copies = []
    for d in range(devices):
        base = (d % 2) * 2 * count
        for j in range(count):
            row = lists[d, start + j]
            dst[base + j : base + j + 1, :] = src[pl.ds(row, 1), :]
            dst[base + count + j : base + count + j + 1, :] = src[pl.ds(row + local, 1), :]
        stage[d, :count, :LANES], stage[d, :count, LANES:] = narrow_rows(dst, base, base + count, count)
        if (d + 1) % group == 0:
            part = pl.ds(d + 1 - group, group)
            copies.append(pltpu.make_async_copy(stage.at[part], out.at[part], sem.at[d // group]))
            copies[-1].start()
    for copy in copies:
        copy.wait()


def widen_rows(x_ref, src):
    local = x_ref.shape[0]

    def widen(c, carry):
        row = pl.multiple_of(c * LANES, LANES)
        src[pl.ds(row, LANES), :] = x_ref[pl.ds(row, LANES), :LANES].astype(F32)
        src[pl.ds(row + local, LANES), :] = x_ref[pl.ds(row, LANES), LANES:].astype(F32)
        return carry

    lax.fori_loop(0, local // LANES, widen, 0)


def send_kernel(
    place_ref, x_hbm, list_ref, out, hot_ref, count_ref, key_ref, x_ref, src, dst, stage, list_s, sem,
    *, groups, shards, first,
):
    devices = groups * shards
    chunks = place_ref.shape[0]
    padded = list_ref.shape[1]
    local, width = x_ref.shape
    rows_in = pltpu.make_async_copy(x_hbm, x_ref, sem.at[0])
    rows_in.start()
    placement = place_ref[...].astype(F32)
    block = floor_div(placement, local)
    within = placement - block * local
    outer = floor_div(block, groups)
    target = (block - outer * groups) * shards + outer
    high = floor_div(within, LANES)
    low = within - high * LANES
    ids = lax.broadcasted_iota(jnp.int32, (devices, LANES), 0).astype(F32)
    for c in range(chunks):
        hot = (ids == target[c : c + 1, :]).astype(F32)
        hot_ref[:, c * LANES : (c + 1) * LANES] = hot.astype(BF16)
    before = lax.broadcasted_iota(jnp.int32, (LANES, LANES), 0) < lax.broadcasted_iota(
        jnp.int32, (LANES, LANES), 1
    )
    prefix = jnp.concatenate(
        [before.astype(F32), jnp.ones((LANES, LANES), F32)], axis=1
    ).astype(BF16)
    for c in range(chunks):
        count_ref[c * devices : (c + 1) * devices, :] = jnp.dot(
            hot_ref[:, c * LANES : (c + 1) * LANES], prefix, preferred_element_type=F32
        )
    carry = jnp.zeros((devices, LANES), F32)
    slots = lax.broadcasted_iota(jnp.int32, (padded, LANES), 0).astype(F32)
    lane = lax.broadcasted_iota(jnp.int32, (1, LANES), 1).astype(F32)
    for c in range(chunks):
        counts = count_ref[c * devices : (c + 1) * devices, :]
        hot = hot_ref[:, c * LANES : (c + 1) * LANES].astype(F32)
        rank = jnp.sum(hot * (counts[:, :LANES] + carry), axis=0, keepdims=True)
        carry = carry + counts[:, LANES:]
        chosen = slots == rank
        values = (high[c : c + 1, :], low[c : c + 1, :], float(c), lane)
        for k, value in enumerate(values):
            key_ref[k * padded : (k + 1) * padded, c * LANES : (c + 1) * LANES] = jnp.where(
                chosen, value, 0.0
            ).astype(BF16)
    codes = lax.dot_general(hot_ref[...], key_ref[...], NT, preferred_element_type=F32)
    source = codes[:, 2 * padded : 3 * padded] * LANES + codes[:, 3 * padded :]
    list_ref[...] = source.astype(jnp.int32)
    lists_in = pltpu.make_async_copy(list_ref, list_s, sem.at[1])
    lists_in.start()
    line = lax.broadcasted_iota(jnp.int32, (TAIL, padded), 0)
    for d in range(devices):
        tail = jnp.where(
            line == 0, codes[d : d + 1, :padded], jnp.where(line == 1, codes[d : d + 1, padded : 2 * padded], 0.0)
        )
        if padded < width:
            tail = jnp.concatenate([tail, jnp.zeros((TAIL, width - padded), F32)], axis=1)
        stage[d, first:, :] = tail.astype(BF16)
    rows_in.wait()
    widen_rows(x_ref, src)
    lists_in.wait()
    fetch_rows(list_s, 0, first, src, dst, stage, out, sem, devices // sem.shape[0])


def send_first(placement, rows, groups, shards, first):
    devices = groups * shards
    local, width = rows.shape
    padded = -(-(local // devices) // LANES) * LANES
    chunks = local // LANES
    vmem = pl.BlockSpec(memory_space=pltpu.VMEM)
    hbm = pl.BlockSpec(memory_space=pl.ANY)
    return pl.pallas_call(
        functools.partial(send_kernel, groups=groups, shards=shards, first=first),
        in_specs=[vmem, hbm],
        out_specs=(vmem, hbm),
        out_shape=(
            jax.ShapeDtypeStruct((devices, padded), jnp.int32),
            jax.ShapeDtypeStruct((devices, first + TAIL, width), BF16),
        ),
        scratch_shapes=[
            pltpu.VMEM((devices, local), BF16),
            pltpu.VMEM((chunks * devices, 2 * LANES), F32),
            pltpu.VMEM((4 * padded, local), BF16),
            pltpu.VMEM((local, width), BF16),
            pltpu.VMEM((2 * local, LANES), F32),
            pltpu.VMEM((4 * first, LANES), F32),
            pltpu.VMEM((devices, first + TAIL, width), BF16),
            pltpu.SMEM((devices, padded), jnp.int32),
            pltpu.SemaphoreType.DMA((4,)),
        ],
        compiler_params=params(),
        name="send_first",
    )(placement.reshape(chunks, LANES), rows)


def rest_kernel(list_ref, x_ref, out, src, dst, stage, sem, *, first):
    widen_rows(x_ref, src)
    fetch_rows(
        list_ref, first, out.shape[1], src, dst, stage, out, sem, list_ref.shape[0] // sem.shape[0]
    )


def send_rest(lists, rows, first, count):
    local, width = rows.shape
    devices = lists.shape[0]
    return pl.pallas_call(
        functools.partial(rest_kernel, first=first),
        in_specs=[pl.BlockSpec(memory_space=pltpu.SMEM), pl.BlockSpec(memory_space=pltpu.VMEM)],
        out_specs=pl.BlockSpec(memory_space=pl.ANY),
        out_shape=jax.ShapeDtypeStruct((devices, count, width), BF16),
        scratch_shapes=[
            pltpu.VMEM((2 * local, LANES), F32),
            pltpu.VMEM((4 * count, LANES), F32),
            pltpu.VMEM((devices, count, width), BF16),
            pltpu.SemaphoreType.DMA((4,)),
        ],
        compiler_params=params(),
        cost_estimate=pl.CostEstimate(
            flops=2_000_000 * devices * count, bytes_accessed=6_000_000, transcendentals=0
        ),
        name="send_rest",
    )(lists, rows)


def slice_weights(standard, feeder_t, logit_t, sharp_ref, offset_ref, logit_ref, weight_ref, total_ref):
    heads = sharp_ref.shape[0]
    slices = offset_ref.shape[1]
    middle = lax.dot_general(feeder_t[...], standard, NT, preferred_element_type=F32).astype(BF16)
    logit_ref[...] = jnp.dot(logit_t[...], middle, preferred_element_type=F32)
    sharp = jnp.broadcast_to(sharp_ref[...], (heads, LANES))
    for start in range(0, weight_ref.shape[1], LANES):
        lanes = pl.ds(start, LANES)
        top = None
        for m in range(slices):
            value = (logit_ref[m * heads : (m + 1) * heads, lanes] + offset_ref[0, m]) * sharp
            top = value if top is None else jnp.maximum(top, value)
        total = None
        for m in range(slices):
            value = (logit_ref[m * heads : (m + 1) * heads, lanes] + offset_ref[0, m]) * sharp
            value = jnp.exp2(value - top)
            logit_ref[m * heads : (m + 1) * heads, lanes] = value
            total = value if total is None else total + value
        scale = 1.0 / total
        for m in range(slices):
            value = logit_ref[m * heads : (m + 1) * heads, lanes] * scale
            weight_ref[m * heads : (m + 1) * heads, lanes] = value.astype(BF16)
            if total_ref is not None:
                total_ref[m * heads : (m + 1) * heads, :] += value


def head_mask(rows, width, heads):
    row_head = lax.broadcasted_iota(jnp.int32, (rows, width), 0) % heads
    return row_head == lax.broadcasted_iota(jnp.int32, (rows, width), 1) // (width // heads)


def repeat_heads(value, width, dims):
    feature = value.shape[dims[0][0][0]]
    pick = lax.broadcasted_iota(jnp.int32, (feature, width), 1) % feature == lax.broadcasted_iota(
        jnp.int32, (feature, width), 0
    )
    return lax.dot_general(
        value, pick.astype(F32), dims, precision=lax.Precision.HIGHEST, preferred_element_type=F32
    )


def sums_kernel(
    x_ref, gain, bias, attribute, feeder_t, partition, sharp_ref, offset_ref,
    packed_ref, logit_t, logit_ref, weight_ref, total_ref, numer_ref,
):
    step = pl.program_id(0)
    heads = sharp_ref.shape[0]
    rows, width = numer_ref.shape
    slices = rows // heads

    @pl.when(step == 0)
    def _():
        total_ref[...] = jnp.zeros_like(total_ref)
        numer_ref[...] = jnp.zeros_like(numer_ref)
        wide = repeat_heads(partition[...].astype(F32), width, TN)
        wide = jnp.broadcast_to(wide[:, None, :], (slices, heads, width))
        logit_t[...] = jnp.where(
            head_mask(rows, width, heads), wide.reshape(rows, width), 0.0
        ).astype(BF16)

    standard = norm_rows(x_ref[...].astype(F32), gain[...], bias[...]).astype(BF16)
    features = jnp.dot(standard, attribute[...], preferred_element_type=F32).astype(BF16)
    slice_weights(
        standard, feeder_t, logit_t, sharp_ref, offset_ref, logit_ref, weight_ref, total_ref
    )
    numer_ref[...] += jnp.dot(weight_ref[...], features, preferred_element_type=F32)

    @pl.when(step == pl.num_programs(0) - 1)
    def _():
        own = jnp.where(head_mask(rows, width, heads), numer_ref[...], 0.0)
        packed_ref[:, :width] = jnp.sum(own.reshape(slices, heads, width), axis=1)
        sums = jnp.sum(total_ref[...], axis=1, keepdims=True)
        lane = lax.broadcasted_iota(jnp.int32, (rows, LANES), 1)
        row_head = lax.broadcasted_iota(jnp.int32, (rows, LANES), 0) % heads
        own = jnp.where(row_head == lane, sums, 0.0)
        packed_ref[:, width:] = jnp.sum(own.reshape(slices, heads, LANES), axis=1)


def local_sums(x, gain, bias, attribute, feeder_t, partition, sharp, offset, block):
    local, width = x.shape
    heads = sharp.shape[0]
    slices = partition.shape[1]
    rows = slices * heads
    return pl.pallas_call(
        sums_kernel,
        grid=(local // block,),
        in_specs=[
            pl.BlockSpec((block, width), lambda i: (i, 0)),
            whole(gain.shape), whole(bias.shape), whole(attribute.shape), whole(feeder_t.shape),
            whole(partition.shape), whole(sharp.shape),
            pl.BlockSpec(memory_space=pltpu.SMEM),
        ],
        out_specs=(whole((slices, width + LANES)), whole((rows, width))),
        out_shape=(
            jax.ShapeDtypeStruct((slices, width + LANES), F32),
            jax.ShapeDtypeStruct((rows, width), BF16),
        ),
        scratch_shapes=[
            pltpu.VMEM((rows, block), F32),
            pltpu.VMEM((rows, block), BF16),
            pltpu.VMEM((rows, LANES), F32),
            pltpu.VMEM((rows, width), F32),
        ],
        compiler_params=params(),
        cost_estimate=pl.CostEstimate(flops=5_000_000_000, bytes_accessed=4_000_000, transcendentals=3_000_000),
        name="local_sums",
    )(x, gain, bias, attribute, feeder_t, partition, sharp, offset)


def attention_kernel(packed_ref, question, lookup, content, mix_t, *, heads):
    highest = lax.Precision.HIGHEST
    slices = packed_ref.shape[0]
    width = packed_ref.shape[1] - LANES
    feature = width // heads
    rows = slices * heads
    spread = (
        lax.broadcasted_iota(jnp.int32, (LANES, width), 0)
        == lax.broadcasted_iota(jnp.int32, (LANES, width), 1) // feature
    ).astype(F32)
    totals = jnp.dot(packed_ref[:, width:], spread, precision=highest, preferred_element_type=F32)
    token = packed_ref[:, :width] / (totals + 1e-05)
    own = (
        lax.broadcasted_iota(jnp.int32, (width, width), 0) // feature
        == lax.broadcasted_iota(jnp.int32, (width, width), 1) // feature
    )

    def per_head(weight):
        wide = repeat_heads(weight[...], width, NN)
        tiled = jnp.broadcast_to(wide[None], (heads, feature, width)).reshape(width, width)
        return jnp.dot(token, jnp.where(own, tiled, 0.0), precision=highest, preferred_element_type=F32)

    query = per_head(question)
    key = per_head(lookup)
    value = per_head(content)
    mask = head_mask(rows, width, heads)
    query = jnp.broadcast_to(query[:, None, :], (slices, heads, width)).reshape(rows, width)
    query = jnp.where(mask, query, 0.0)
    scores = lax.dot_general(query, key, NT, precision=highest, preferred_element_type=F32)
    scores = scores * (1.0 / math.sqrt(feature))
    scores = jnp.exp(scores - jnp.max(scores, axis=-1, keepdims=True))
    attention = scores / jnp.sum(scores, axis=-1, keepdims=True)
    mixed = jnp.dot(attention, value, precision=highest, preferred_element_type=F32)
    mix_t[...] = jnp.where(mask, mixed, 0.0).T.astype(BF16)


def slice_attention(packed, question, lookup, content, heads):
    slices = packed.shape[0]
    width = packed.shape[1] - LANES
    return pl.pallas_call(
        functools.partial(attention_kernel, heads=heads),
        out_shape=jax.ShapeDtypeStruct((width, slices * heads), BF16),
        compiler_params=params(),
        name="slice_attention",
    )(packed, question, lookup, content)


def finish_kernel(
    pos_hbm, x_ref, gain, bias, feeder_t, logit_t, sharp_ref, offset_ref, mix_t, emitted, emitted_offset,
    gain2, bias2, entry, entry_offset, leave, leave_offset, *refs, start, per, follows, last,
):
    refs = list(refs)
    before = refs.pop(0) if follows else None
    out_ref, logit_ref, weight_ref, res, dst, pos_ref, sem, pos_sem = refs[:8]
    step = pl.program_id(0)
    sources = x_ref.shape[0]
    block = sources * per
    local = dst.shape[0] // 2

    slots_in = pltpu.make_async_copy(
        pos_hbm.at[pl.ds(pl.multiple_of(step * sources, 8), sources)], pos_ref, pos_sem.at[0]
    )
    slots_in.start()

    def handover(inward):
        if inward:
            return pltpu.make_async_copy(before, dst, sem.at[0])
        return pltpu.make_async_copy(dst, out_ref, sem.at[0])

    if follows:

        @pl.when(step == 0)
        def _():
            handover(True).start()

    x = jnp.concatenate([x_ref[s, :per, :] for s in range(sources)], axis=0).astype(F32)
    standard = norm_rows(x, gain[...], bias[...]).astype(BF16)
    slice_weights(standard, feeder_t, logit_t, sharp_ref, offset_ref, logit_ref, weight_ref, None)
    blended_t = jnp.dot(mix_t[...], weight_ref[...], preferred_element_type=F32)
    blended = blended_t.T.astype(BF16)
    hidden = x + jnp.dot(blended, emitted[...], preferred_element_type=F32) + emitted_offset[...]
    normed = norm_rows(hidden, gain2[...], bias2[...]).astype(BF16)
    inner = jnp.dot(normed, entry[...], preferred_element_type=F32) + entry_offset[...]
    active = (inner * (1.0 + lax.erf(inner * math.sqrt(0.5)))).astype(BF16)
    leaving = jnp.dot(active, leave[...], preferred_element_type=F32)
    result = hidden + 0.5 * leaving + leave_offset[...]
    res[:block, :] = result[:, :LANES]
    res[block:, :] = result[:, LANES:]
    if follows:

        @pl.when(step == 0)
        def _():
            handover(True).wait()

    slots_in.wait()
    for source in range(sources):
        for j in range(per):
            slot = pos_ref[source, start + j]
            row = source * per + j
            dst[pl.ds(slot, 1), :] = res[row : row + 1, :]
            dst[pl.ds(slot + local, 1), :] = res[row + block : row + block + 1, :]

    @pl.when(step == pl.num_programs(0) - 1)
    def _():
        if not last:
            handover(False).start()
            handover(False).wait()
        else:
            stage = refs[8]
            parts = sem.shape[0]
            size = local // parts
            copies = []
            for q in range(parts):

                def narrow(c, carry, q=q):
                    row = pl.multiple_of(q * size + c * LANES, LANES)
                    stage[pl.ds(row, LANES), :LANES] = dst[pl.ds(row, LANES), :].astype(BF16)
                    stage[pl.ds(row, LANES), LANES:] = dst[pl.ds(row + local, LANES), :].astype(BF16)
                    return carry

                lax.fori_loop(0, size // LANES, narrow, 0)
                rows = pl.ds(q * size, size)
                copies.append(pltpu.make_async_copy(stage.at[rows], out_ref.at[rows], sem.at[q]))
                copies[-1].start()
            for copy in copies:
                copy.wait()


def finish_rows(positions, arrived, weights, offset, mix_t, rest, before, local, start, per, last):
    devices, stride, width = arrived.shape
    rows = mix_t.shape[1]
    sources = max(
        k for k in range(8, devices + 1, 8)
        if devices % k == 0 and k * per <= BLOCK and k * per % LANES == 0
    )
    block = sources * per
    follows = before is not None
    shape = (local, width) if last else (2 * local, LANES)
    return pl.pallas_call(
        functools.partial(finish_kernel, start=start, per=per, follows=follows, last=last),
        grid=(devices // sources,),
        in_specs=[
            pl.BlockSpec(memory_space=pl.ANY),
            pl.BlockSpec((sources, stride, width), lambda i: (i, 0, 0)),
            *[whole(w.shape) for w in weights],
            pl.BlockSpec(memory_space=pltpu.SMEM),
            whole(mix_t.shape),
            *[whole(w.shape) for w in rest],
            *([pl.BlockSpec(memory_space=pl.ANY)] if follows else []),
        ],
        out_specs=pl.BlockSpec(memory_space=pl.ANY),
        out_shape=jax.ShapeDtypeStruct(shape, BF16 if last else F32),
        scratch_shapes=[
            pltpu.VMEM((rows, block), F32),
            pltpu.VMEM((rows, block), BF16),
            pltpu.VMEM((2 * block, LANES), F32),
            pltpu.VMEM((2 * local, LANES), F32),
            pltpu.SMEM((sources, positions.shape[1]), jnp.int32),
            pltpu.SemaphoreType.DMA((4 if last else 1,)),
            pltpu.SemaphoreType.DMA((1,)),
            *([pltpu.VMEM((local, width), BF16)] if last else []),
        ],
        compiler_params=params(),
        cost_estimate=pl.CostEstimate(
            flops=2_000_000 * devices * per, bytes_accessed=8_000_000, transcendentals=1000 * devices * per
        ),
    )(positions, arrived, *weights, offset, mix_t, *rest, *([before] if follows else []))


def sum_plane(value, shards):
    step = 1
    while step < shards:
        value = value + lax.ppermute(value, "pts", [(i, i ^ step) for i in range(shards)])
        step *= 2
    return value


def sum_head(value, groups):
    others = [lax.ppermute(value, "head", [(i, i ^ k) for i in range(groups)]) for k in range(1, groups)]
    for other in others:
        value = value + other
    return value


def body(
    layer_inputs_trainorder,
    inference_placement,
    initial_layernorm_gain,
    initial_layernorm_offset,
    attribute_projection,
    assignment_feeder_projection,
    partition_projection,
    partition_offset,
    softmax_sharpness,
    partition_question_map,
    partition_lookup_map,
    partition_content_map,
    emitted_projection,
    emitted_offset,
    latter_layernorm_gain,
    latter_layernorm_offset,
    perceptron_entry_map,
    perceptron_entry_offset,
    perceptron_exit_map,
    perceptron_exit_offset,
):
    groups = lax.axis_size("head")
    shards = lax.axis_size("pts")
    devices = groups * shards
    local, width = layer_inputs_trainorder.shape
    feature, _ = partition_projection.shape
    heads = width // feature
    per = local // devices
    block = 768 if local % 768 == 0 else LANES
    first = per * 7 // 12 // 8 * 8
    second = per - first

    def exchange(rows):
        return lax.all_to_all(rows, ("head", "pts"), split_axis=0, concat_axis=0, tiled=True)

    mates = [
        lax.ppermute(softmax_sharpness, "head", [(i, i ^ k) for i in range(groups)])
        for k in range(1, groups)
    ]
    lists, one = send_first(inference_placement, layer_inputs_trainorder, groups, shards, first)
    *mates, one = lax.optimization_barrier((*mates, one))
    arrived_one = exchange(one)
    two = send_rest(lists, layer_inputs_trainorder, first, second)

    place = lax.axis_index("head")
    order = jnp.arange(groups)[:, None]
    sharp = jnp.where(order == place, softmax_sharpness[None], 0.0)
    for k, mate in enumerate(mates, 1):
        sharp = jnp.where(order == (place ^ k), mate[None], sharp)
    sharp = (LOG2E / sharp).reshape(heads, 1)
    gain = initial_layernorm_gain[None]
    bias = initial_layernorm_offset[None]
    feeder_t = assignment_feeder_projection.T
    offset = partition_offset[None]
    packed, logit_t = local_sums(
        layer_inputs_trainorder, gain, bias, attribute_projection, feeder_t, partition_projection, sharp,
        offset, block,
    )
    packed = sum_plane(packed, shards)
    _, arrived_one, two = lax.optimization_barrier((packed, arrived_one, two))
    arrived_two = exchange(two)
    packed = sum_head(packed, groups)

    codes = lax.optimization_barrier(arrived_one[:, first:, :])[:, :2, :].astype(F32)
    arrived_at = (codes[:, 0] * LANES + codes[:, 1]).astype(jnp.int32)
    mix_t = slice_attention(
        packed, partition_question_map, partition_lookup_map, partition_content_map, heads
    )
    weights = (gain, bias, feeder_t, logit_t, sharp)
    rest = (
        emitted_projection, emitted_offset[None], latter_layernorm_gain[None], latter_layernorm_offset[None],
        perceptron_entry_map, perceptron_entry_offset[None],
        perceptron_exit_map, perceptron_exit_offset[None],
    )
    served = finish_rows(
        arrived_at, arrived_one, weights, offset, mix_t, rest, None, local, 0, first, False
    )
    served = finish_rows(
        arrived_at, arrived_two, weights, offset, mix_t, rest, served, local, first, second, True
    )
    return served[None]


def solution(mesh):
    rows = P(("head", "pts"))
    placed = (P(("head", "pts"), None), rows, *[P()] * 6, P("head"), *[P()] * 11)

    return jax.shard_map(body, mesh=mesh, in_specs=placed, out_specs=P("pts", "head", None), check_vma=False)
```

```python
import functools
import math

import jax
import jax.numpy as jnp
from jax import lax
from jax.experimental import pallas as pl
from jax.experimental.pallas import tpu as pltpu
from jax.sharding import PartitionSpec as P


F32 = jnp.float32
BF16 = jnp.bfloat16
LANES = 128
TAIL = 8
SUBLANES = 8
BLOCK = 1024
EPS_NORM = 1e-05
LOG2E = math.log2(math.e)
NT = (((1,), (1,)), ((), ()))
TN = (((0,), (0,)), ((), ()))
NN = (((1,), (0,)), ((), ()))
VMEM = 56 * 1024 * 1024


def whole(shape):
    return pl.BlockSpec(shape, lambda *_: (0,) * len(shape))


def params():
    return pltpu.CompilerParams(vmem_limit_bytes=VMEM)


def floor_div(value, divisor):
    return jnp.floor((value + 0.5) * (1.0 / divisor))


def norm_rows(row_block, gain, bias):
    mean = jnp.mean(row_block, axis=-1, keepdims=True)
    centred = row_block - mean
    spread = jnp.mean(centred * centred, axis=-1, keepdims=True)
    return centred * lax.rsqrt(spread + EPS_NORM) * gain + bias


def pick_rows(src, base, rows):
    sub = lax.broadcasted_iota(jnp.int32, (SUBLANES, LANES), 0)
    merged = src[pl.ds(rows[0] + (base + SUBLANES), SUBLANES), :]
    for j in range(1, SUBLANES):
        merged = jnp.where(sub == j, src[pl.ds(rows[j] + (base + SUBLANES - j), SUBLANES), :], merged)
    return merged.astype(BF16)


def fetch_rows(lists, d, start, counts, src, stages):
    local = src.shape[0] // 2 - SUBLANES
    for stage, count in zip(stages, counts):
        for first in range(0, count, SUBLANES):
            rows = [lists[d, start + first + j] for j in range(SUBLANES)]
            stage[d, first : first + SUBLANES, :LANES] = pick_rows(src, 0, rows)
            stage[d, first : first + SUBLANES, LANES:] = pick_rows(src, local, rows)
        start += count


def widen_rows(x_ref, src):
    local = x_ref.shape[0]

    def widen(c, carry):
        row = pl.multiple_of(c * LANES, LANES)
        src[pl.ds(row + SUBLANES, LANES), :] = x_ref[pl.ds(row, LANES), :LANES].astype(F32)
        src[pl.ds(row + (local + SUBLANES), LANES), :] = x_ref[pl.ds(row, LANES), LANES:].astype(F32)
        return carry

    lax.fori_loop(0, local // LANES, widen, 0)


def send_kernel(
    place_ref, x_hbm, list_ref, out, hot_ref, count_ref, key_ref, x_ref, src, stage, list_s, sem,
    *, groups, shards, first,
):
    devices = groups * shards
    chunks = place_ref.shape[0]
    local, width = x_ref.shape
    per = local // devices
    rows_in = pltpu.make_async_copy(x_hbm, x_ref, sem.at[0])
    rows_in.start()
    placement = place_ref[...].astype(F32)
    block = floor_div(placement, local)
    within = placement - block * local
    outer = floor_div(block, groups)
    target = (block - outer * groups) * shards + outer
    high = floor_div(within, LANES)
    low = within - high * LANES
    ids = lax.broadcasted_iota(jnp.int32, (devices, LANES), 0).astype(F32)
    for c in range(chunks):
        hot = (ids == target[c : c + 1, :]).astype(F32)
        hot_ref[:, c * LANES : (c + 1) * LANES] = hot.astype(BF16)
    before = lax.broadcasted_iota(jnp.int32, (LANES, LANES), 0) < lax.broadcasted_iota(
        jnp.int32, (LANES, LANES), 1
    )
    prefix = jnp.concatenate(
        [before.astype(F32), jnp.ones((LANES, LANES), F32)], axis=1
    ).astype(BF16)
    for c in range(chunks):
        count_ref[c * devices : (c + 1) * devices, :] = jnp.dot(
            hot_ref[:, c * LANES : (c + 1) * LANES], prefix, preferred_element_type=F32
        )
    carry = jnp.zeros((devices, LANES), F32)
    slots = lax.broadcasted_iota(jnp.int32, (per, LANES), 0).astype(F32).astype(BF16)
    lane = lax.broadcasted_iota(jnp.int32, (1, LANES), 1).astype(F32)
    zero = jnp.zeros((per, LANES), BF16)
    for c in range(chunks):
        counts = count_ref[c * devices : (c + 1) * devices, :]
        hot = hot_ref[:, c * LANES : (c + 1) * LANES].astype(F32)
        rank = jnp.sum(hot * (counts[:, :LANES] + carry), axis=0, keepdims=True)
        carry = carry + counts[:, LANES:]
        chosen = slots == jnp.broadcast_to(rank, (per, LANES)).astype(BF16)
        values = (high[c : c + 1, :], low[c : c + 1, :], jnp.full((1, LANES), float(c), F32), lane)
        for k, value in enumerate(values):
            key_ref[k * per : (k + 1) * per, c * LANES : (c + 1) * LANES] = jnp.where(
                chosen, jnp.broadcast_to(value, (per, LANES)).astype(BF16), zero
            )
    codes = lax.dot_general(hot_ref[...], key_ref[...], NT, preferred_element_type=F32)
    source = codes[:, 2 * per : 3 * per] * LANES + codes[:, 3 * per :]
    list_ref[...] = jnp.zeros_like(list_ref)
    list_ref[:, :per] = source.astype(jnp.int32)
    lists_in = pltpu.make_async_copy(list_ref, list_s, sem.at[1])
    lists_in.start()
    line = lax.broadcasted_iota(jnp.int32, (TAIL, per), 0)
    label_high, label_low = codes[:, :per], codes[:, per : 2 * per]
    stage[:, first:, :] = jnp.zeros((devices, TAIL, width), BF16)
    for d in range(devices):
        tail = jnp.where(line == 0, label_high[d : d + 1], jnp.where(line == 1, label_low[d : d + 1], 0.0))
        stage[d, first:, :per] = tail.astype(BF16)
    rows_in.wait()
    widen_rows(x_ref, src)
    lists_in.wait()
    copies = []
    group = devices // sem.shape[0]
    for g in range(sem.shape[0]):

        def fetch(d, carry):
            fetch_rows(list_s, d, 0, (first,), src, (stage,))
            return carry

        lax.fori_loop(g * group, (g + 1) * group, fetch, 0)
        part = pl.ds(g * group, group)
        copies.append(pltpu.make_async_copy(stage.at[part], out.at[part], sem.at[g]))
        copies[-1].start()
    for copy in copies:
        copy.wait()


def send_first(placement, rows, groups, shards, first):
    devices = groups * shards
    local, width = rows.shape
    per = local // devices
    padded = -(-per // LANES) * LANES
    chunks = local // LANES
    vmem = pl.BlockSpec(memory_space=pltpu.VMEM)
    hbm = pl.BlockSpec(memory_space=pl.ANY)
    return pl.pallas_call(
        functools.partial(send_kernel, groups=groups, shards=shards, first=first),
        in_specs=[vmem, hbm],
        out_specs=(vmem, hbm),
        out_shape=(
            jax.ShapeDtypeStruct((devices, padded), jnp.int32),
            jax.ShapeDtypeStruct((devices, first + TAIL, width), BF16),
        ),
        scratch_shapes=[
            pltpu.VMEM((devices, local), BF16),
            pltpu.VMEM((chunks * devices, 2 * LANES), F32),
            pltpu.VMEM((4 * per, local), BF16),
            pltpu.VMEM((local, width), BF16),
            pltpu.VMEM((2 * (local + SUBLANES), LANES), F32),
            pltpu.VMEM((devices, first + TAIL, width), BF16),
            pltpu.SMEM((devices, padded), jnp.int32),
            pltpu.SemaphoreType.DMA((4,)),
        ],
        compiler_params=params(),
        name="send_first",
    )(placement.reshape(chunks, LANES), rows)


def rest_kernel(list_ref, x_ref, one, two, src, *, first):
    widen_rows(x_ref, src)

    def fetch(d, carry):
        fetch_rows(list_ref, d, first, (one.shape[1], two.shape[1]), src, (one, two))
        return carry

    lax.fori_loop(0, list_ref.shape[0], fetch, 0)


def send_rest(lists, rows, first, counts):
    local, width = rows.shape
    devices = lists.shape[0]
    return pl.pallas_call(
        functools.partial(rest_kernel, first=first),
        in_specs=[pl.BlockSpec(memory_space=pltpu.SMEM), pl.BlockSpec(memory_space=pltpu.VMEM)],
        out_shape=[jax.ShapeDtypeStruct((devices, n, width), BF16) for n in counts],
        scratch_shapes=[pltpu.VMEM((2 * (local + SUBLANES), LANES), F32)],
        compiler_params=params(),
        cost_estimate=pl.CostEstimate(
            flops=2_000_000 * devices * sum(counts), bytes_accessed=6_000_000, transcendentals=0
        ),
        name="send_rest",
    )(lists, rows)


def slice_weights(standard, feeder_t, logit_t, sharp_ref, offset_ref, logit_ref, weight_ref, total_ref):
    heads = sharp_ref.shape[0]
    slices = offset_ref.shape[1]
    middle = lax.dot_general(feeder_t[...], standard, NT, preferred_element_type=F32).astype(BF16)
    logit_ref[...] = jnp.dot(logit_t[...], middle, preferred_element_type=F32)
    sharp = jnp.broadcast_to(sharp_ref[...], (heads, LANES))
    for start in range(0, weight_ref.shape[1], LANES):
        lanes = pl.ds(start, LANES)
        top = None
        for m in range(slices):
            value = (logit_ref[m * heads : (m + 1) * heads, lanes] + offset_ref[0, m]) * sharp
            top = value if top is None else jnp.maximum(top, value)
        total = None
        for m in range(slices):
            value = (logit_ref[m * heads : (m + 1) * heads, lanes] + offset_ref[0, m]) * sharp
            value = jnp.exp2(value - top)
            logit_ref[m * heads : (m + 1) * heads, lanes] = value
            total = value if total is None else total + value
        scale = 1.0 / total
        for m in range(slices):
            value = logit_ref[m * heads : (m + 1) * heads, lanes] * scale
            weight_ref[m * heads : (m + 1) * heads, lanes] = value.astype(BF16)
            if total_ref is not None:
                total_ref[m * heads : (m + 1) * heads, :] += value


def head_mask(rows, width, heads):
    row_head = lax.broadcasted_iota(jnp.int32, (rows, width), 0) % heads
    return row_head == lax.broadcasted_iota(jnp.int32, (rows, width), 1) // (width // heads)


def repeat_heads(value, width, dims):
    feature = value.shape[dims[0][0][0]]
    pick = lax.broadcasted_iota(jnp.int32, (feature, width), 1) % feature == lax.broadcasted_iota(
        jnp.int32, (feature, width), 0
    )
    return lax.dot_general(
        value, pick.astype(F32), dims, precision=lax.Precision.HIGHEST, preferred_element_type=F32
    )


def sums_kernel(
    x_ref, gain, bias, attribute, feeder_t, partition, sharp_ref, offset_ref,
    packed_ref, logit_t, logit_ref, weight_ref, total_ref, numer_ref,
):
    step = pl.program_id(0)
    heads = sharp_ref.shape[0]
    rows, width = numer_ref.shape
    slices = rows // heads

    @pl.when(step == 0)
    def _():
        total_ref[...] = jnp.zeros_like(total_ref)
        numer_ref[...] = jnp.zeros_like(numer_ref)
        wide = repeat_heads(partition[...].astype(F32), width, TN)
        wide = jnp.broadcast_to(wide[:, None, :], (slices, heads, width))
        logit_t[...] = jnp.where(
            head_mask(rows, width, heads), wide.reshape(rows, width), 0.0
        ).astype(BF16)

    standard = norm_rows(x_ref[...].astype(F32), gain[...], bias[...]).astype(BF16)
    features = jnp.dot(standard, attribute[...], preferred_element_type=F32).astype(BF16)
    slice_weights(
        standard, feeder_t, logit_t, sharp_ref, offset_ref, logit_ref, weight_ref, total_ref
    )
    numer_ref[...] += jnp.dot(weight_ref[...], features, preferred_element_type=F32)

    @pl.when(step == pl.num_programs(0) - 1)
    def _():
        own = jnp.where(head_mask(rows, width, heads), numer_ref[...], 0.0)
        packed_ref[:, :width] = jnp.sum(own.reshape(slices, heads, width), axis=1)
        sums = jnp.sum(total_ref[...], axis=1, keepdims=True)
        lane = lax.broadcasted_iota(jnp.int32, (rows, LANES), 1)
        row_head = lax.broadcasted_iota(jnp.int32, (rows, LANES), 0) % heads
        own = jnp.where(row_head == lane, sums, 0.0)
        packed_ref[:, width:] = jnp.sum(own.reshape(slices, heads, LANES), axis=1)


def local_sums(x, gain, bias, attribute, feeder_t, partition, sharp, offset, block):
    local, width = x.shape
    heads = sharp.shape[0]
    slices = partition.shape[1]
    rows = slices * heads
    return pl.pallas_call(
        sums_kernel,
        grid=(local // block,),
        in_specs=[
            pl.BlockSpec((block, width), lambda i: (i, 0)),
            whole(gain.shape), whole(bias.shape), whole(attribute.shape), whole(feeder_t.shape),
            whole(partition.shape), whole(sharp.shape),
            pl.BlockSpec(memory_space=pltpu.SMEM),
        ],
        out_specs=(whole((slices, width + LANES)), whole((rows, width))),
        out_shape=(
            jax.ShapeDtypeStruct((slices, width + LANES), F32),
            jax.ShapeDtypeStruct((rows, width), BF16),
        ),
        scratch_shapes=[
            pltpu.VMEM((rows, block), F32),
            pltpu.VMEM((rows, block), BF16),
            pltpu.VMEM((rows, LANES), F32),
            pltpu.VMEM((rows, width), F32),
        ],
        compiler_params=params(),
        cost_estimate=pl.CostEstimate(flops=5_000_000_000, bytes_accessed=4_000_000, transcendentals=3_000_000),
        name="local_sums",
    )(x, gain, bias, attribute, feeder_t, partition, sharp, offset)


def attention_kernel(packed_ref, question, lookup, content, mix_t, *, heads):
    highest = lax.Precision.HIGHEST
    slices = packed_ref.shape[0]
    width = packed_ref.shape[1] - LANES
    feature = width // heads
    rows = slices * heads
    spread = (
        lax.broadcasted_iota(jnp.int32, (LANES, width), 0)
        == lax.broadcasted_iota(jnp.int32, (LANES, width), 1) // feature
    ).astype(F32)
    totals = jnp.dot(packed_ref[:, width:], spread, precision=highest, preferred_element_type=F32)
    token = packed_ref[:, :width] / (totals + 1e-05)
    own = (
        lax.broadcasted_iota(jnp.int32, (width, width), 0) // feature
        == lax.broadcasted_iota(jnp.int32, (width, width), 1) // feature
    )

    def per_head(weight):
        wide = repeat_heads(weight[...], width, NN)
        tiled = jnp.broadcast_to(wide[None], (heads, feature, width)).reshape(width, width)
        return jnp.dot(token, jnp.where(own, tiled, 0.0), precision=highest, preferred_element_type=F32)

    query = per_head(question)
    key = per_head(lookup)
    value = per_head(content)
    mask = head_mask(rows, width, heads)
    query = jnp.broadcast_to(query[:, None, :], (slices, heads, width)).reshape(rows, width)
    query = jnp.where(mask, query, 0.0)
    scores = lax.dot_general(query, key, NT, precision=highest, preferred_element_type=F32)
    scores = scores * (1.0 / math.sqrt(feature))
    scores = jnp.exp(scores - jnp.max(scores, axis=-1, keepdims=True))
    attention = scores / jnp.sum(scores, axis=-1, keepdims=True)
    mixed = jnp.dot(attention, value, precision=highest, preferred_element_type=F32)
    mix_t[...] = jnp.where(mask, mixed, 0.0).T.astype(BF16)


def slice_attention(packed, question, lookup, content, heads):
    slices = packed.shape[0]
    width = packed.shape[1] - LANES
    return pl.pallas_call(
        functools.partial(attention_kernel, heads=heads),
        out_shape=jax.ShapeDtypeStruct((width, slices * heads), BF16),
        compiler_params=params(),
        name="slice_attention",
    )(packed, question, lookup, content)


def finish_kernel(
    pos_hbm, x_ref, gain, bias, feeder_t, logit_t, sharp_ref, offset_ref, mix_t, emitted, emitted_offset,
    gain2, bias2, entry, entry_offset, leave, leave_offset, *refs, start, per, follows, last,
):
    refs = list(refs)
    before = refs.pop(0) if follows else None
    out_ref, logit_ref, weight_ref, res, dst, pos_ref, sem, pos_sem = refs[:8]
    step = pl.program_id(0)
    sources = x_ref.shape[0]
    block = sources * per
    local = dst.shape[0] // 2

    slots_in = pltpu.make_async_copy(
        pos_hbm.at[pl.ds(pl.multiple_of(step * sources, 8), sources)], pos_ref, pos_sem.at[0]
    )
    slots_in.start()

    def handover(inward):
        if inward:
            return pltpu.make_async_copy(before, dst, sem.at[0])
        return pltpu.make_async_copy(dst, out_ref, sem.at[0])

    if follows:

        @pl.when(step == 0)
        def _():
            handover(True).start()

    x = jnp.concatenate([x_ref[s, :per, :] for s in range(sources)], axis=0).astype(F32)
    standard = norm_rows(x, gain[...], bias[...]).astype(BF16)
    slice_weights(standard, feeder_t, logit_t, sharp_ref, offset_ref, logit_ref, weight_ref, None)
    blended_t = jnp.dot(mix_t[...], weight_ref[...], preferred_element_type=F32)
    blended = blended_t.T.astype(BF16)
    hidden = x + jnp.dot(blended, emitted[...], preferred_element_type=F32) + emitted_offset[...]
    normed = norm_rows(hidden, gain2[...], bias2[...]).astype(BF16)
    inner = jnp.dot(normed, entry[...], preferred_element_type=F32) + entry_offset[...]
    active = (inner * (1.0 + lax.erf(inner * math.sqrt(0.5)))).astype(BF16)
    leaving = jnp.dot(active, leave[...], preferred_element_type=F32)
    result = hidden + 0.5 * leaving + leave_offset[...]
    res[:block, :] = result[:, :LANES]
    res[block:, :] = result[:, LANES:]
    if follows:

        @pl.when(step == 0)
        def _():
            handover(True).wait()

    slots_in.wait()
    for source in range(sources):
        for j in range(per):
            slot = pos_ref[source, start + j]
            row = source * per + j
            dst[pl.ds(slot, 1), :] = res[row : row + 1, :]
            dst[pl.ds(slot + local, 1), :] = res[row + block : row + block + 1, :]

    @pl.when(step == pl.num_programs(0) - 1)
    def _():
        if not last:
            handover(False).start()
            handover(False).wait()
        else:
            stage = refs[8]
            parts = sem.shape[0]
            size = local // parts
            copies = []
            for q in range(parts):

                def narrow(c, carry, q=q):
                    row = pl.multiple_of(q * size + c * LANES, LANES)
                    stage[pl.ds(row, LANES), :LANES] = dst[pl.ds(row, LANES), :].astype(BF16)
                    stage[pl.ds(row, LANES), LANES:] = dst[pl.ds(row + local, LANES), :].astype(BF16)
                    return carry

                lax.fori_loop(0, size // LANES, narrow, 0)
                rows = pl.ds(q * size, size)
                copies.append(pltpu.make_async_copy(stage.at[rows], out_ref.at[rows], sem.at[q]))
                copies[-1].start()
            for copy in copies:
                copy.wait()


def finish_rows(positions, arrived, weights, offset, mix_t, rest, before, local, start, per, last):
    devices, stride, width = arrived.shape
    rows = mix_t.shape[1]
    sources = max(
        k for k in range(8, devices + 1, 8)
        if devices % k == 0 and k * per <= BLOCK and k * per % LANES == 0
    )
    block = sources * per
    follows = before is not None
    shape = (local, width) if last else (2 * local, LANES)
    return pl.pallas_call(
        functools.partial(finish_kernel, start=start, per=per, follows=follows, last=last),
        grid=(devices // sources,),
        in_specs=[
            pl.BlockSpec(memory_space=pl.ANY),
            pl.BlockSpec((sources, stride, width), lambda i: (i, 0, 0)),
            *[whole(w.shape) for w in weights],
            pl.BlockSpec(memory_space=pltpu.SMEM),
            whole(mix_t.shape),
            *[whole(w.shape) for w in rest],
            *([pl.BlockSpec(memory_space=pl.ANY)] if follows else []),
        ],
        out_specs=pl.BlockSpec(memory_space=pl.ANY),
        out_shape=jax.ShapeDtypeStruct(shape, BF16 if last else F32),
        scratch_shapes=[
            pltpu.VMEM((rows, block), F32),
            pltpu.VMEM((rows, block), BF16),
            pltpu.VMEM((2 * block, LANES), F32),
            pltpu.VMEM((2 * local, LANES), F32),
            pltpu.SMEM((sources, positions.shape[1]), jnp.int32),
            pltpu.SemaphoreType.DMA((4 if last else 1,)),
            pltpu.SemaphoreType.DMA((1,)),
            *([pltpu.VMEM((local, width), BF16)] if last else []),
        ],
        compiler_params=params(),
        cost_estimate=pl.CostEstimate(
            flops=2_000_000 * devices * per, bytes_accessed=8_000_000, transcendentals=1000 * devices * per
        ),
    )(positions, arrived, *weights, offset, mix_t, *rest, *([before] if follows else []))


def sum_plane(value, shards):
    step = 1
    while step < shards:
        value = value + lax.ppermute(value, "pts", [(i, i ^ step) for i in range(shards)])
        step *= 2
    return value


def sum_head(value, groups):
    others = [lax.ppermute(value, "head", [(i, i ^ k) for i in range(groups)]) for k in range(1, groups)]
    for other in others:
        value = value + other
    return value


def body(
    layer_inputs_trainorder,
    inference_placement,
    initial_layernorm_gain,
    initial_layernorm_offset,
    attribute_projection,
    assignment_feeder_projection,
    partition_projection,
    partition_offset,
    softmax_sharpness,
    partition_question_map,
    partition_lookup_map,
    partition_content_map,
    emitted_projection,
    emitted_offset,
    latter_layernorm_gain,
    latter_layernorm_offset,
    perceptron_entry_map,
    perceptron_entry_offset,
    perceptron_exit_map,
    perceptron_exit_offset,
):
    groups = lax.axis_size("head")
    shards = lax.axis_size("pts")
    devices = groups * shards
    local, width = layer_inputs_trainorder.shape
    feature, _ = partition_projection.shape
    heads = width // feature
    per = local // devices
    block = 768 if local % 768 == 0 else LANES
    first = per // 2 // 8 * 8
    second = per // 3 // 8 * 8
    third = per - first - second

    def exchange(rows):
        return lax.all_to_all(rows, ("head", "pts"), split_axis=0, concat_axis=0, tiled=True)

    mates = [
        lax.ppermute(softmax_sharpness, "head", [(i, i ^ k) for i in range(groups)])
        for k in range(1, groups)
    ]
    lists, one = send_first(inference_placement, layer_inputs_trainorder, groups, shards, first)
    *mates, one = lax.optimization_barrier((*mates, one))
    arrived_one = exchange(one)
    two, three = send_rest(lists, layer_inputs_trainorder, first, (second, third))

    place = lax.axis_index("head")
    order = jnp.arange(groups)[:, None]
    sharp = jnp.where(order == place, softmax_sharpness[None], 0.0)
    for k, mate in enumerate(mates, 1):
        sharp = jnp.where(order == (place ^ k), mate[None], sharp)
    sharp = (LOG2E / sharp).reshape(heads, 1)
    gain = initial_layernorm_gain[None]
    bias = initial_layernorm_offset[None]
    feeder_t = assignment_feeder_projection.T
    offset = partition_offset[None]
    packed, logit_t = local_sums(
        layer_inputs_trainorder, gain, bias, attribute_projection, feeder_t, partition_projection, sharp,
        offset, block,
    )
    packed = sum_plane(packed, shards)
    _, arrived_one, two = lax.optimization_barrier((packed, arrived_one, two))
    arrived_two = exchange(two)
    packed = sum_head(packed, groups)

    codes = lax.optimization_barrier(arrived_one[:, first:, :])[:, :2, :].astype(F32)
    arrived_at = (codes[:, 0] * LANES + codes[:, 1]).astype(jnp.int32)
    mix_t = slice_attention(
        packed, partition_question_map, partition_lookup_map, partition_content_map, heads
    )
    weights = (gain, bias, feeder_t, logit_t, sharp)
    rest = (
        emitted_projection, emitted_offset[None], latter_layernorm_gain[None], latter_layernorm_offset[None],
        perceptron_entry_map, perceptron_entry_offset[None],
        perceptron_exit_map, perceptron_exit_offset[None],
    )
    served = finish_rows(
        arrived_at, arrived_one, weights, offset, mix_t, rest, None, local, 0, first, False
    )
    served, arrived_two, three = lax.optimization_barrier((served, arrived_two, three))
    arrived_three = exchange(three)
    served = finish_rows(
        arrived_at, arrived_two, weights, offset, mix_t, rest, served, local, first, second, False
    )
    served = finish_rows(
        arrived_at, arrived_three, weights, offset, mix_t, rest, served, local, first + second, third, True
    )
    return served[None]


def solution(mesh):
    rows = P(("head", "pts"))
    placed = (P(("head", "pts"), None), rows, *[P()] * 6, P("head"), *[P()] * 11)

    return jax.shard_map(body, mesh=mesh, in_specs=placed, out_specs=P("pts", "head", None), check_vma=False)
```

```python
import functools
import math

import jax
import jax.numpy as jnp
from jax import lax
from jax.experimental import pallas as pl
from jax.experimental.pallas import tpu as pltpu
from jax.sharding import PartitionSpec as P


F32 = jnp.float32
BF16 = jnp.bfloat16
LANES = 128
TAIL = 8
SUBLANES = 8
BLOCK = 1024
EPS_NORM = 1e-05
LOG2E = math.log2(math.e)
NT = (((1,), (1,)), ((), ()))
TN = (((0,), (0,)), ((), ()))
NN = (((1,), (0,)), ((), ()))
VMEM = 56 * 1024 * 1024


def whole(shape):
    return pl.BlockSpec(shape, lambda *_: (0,) * len(shape))


def params():
    return pltpu.CompilerParams(vmem_limit_bytes=VMEM)


def floor_div(value, divisor):
    return jnp.floor((value + 0.5) * (1.0 / divisor))


def norm_rows(row_block, gain, bias):
    mean = jnp.mean(row_block, axis=-1, keepdims=True)
    centred = row_block - mean
    spread = jnp.mean(centred * centred, axis=-1, keepdims=True)
    return centred * lax.rsqrt(spread + EPS_NORM) * gain + bias


def pick_rows(src, places):
    pair = lax.broadcasted_iota(jnp.int32, (SUBLANES, LANES), 0) // 2
    merged = src[pl.ds(places[0] + SUBLANES, SUBLANES), :]
    for j in range(1, len(places)):
        merged = jnp.where(pair == j, src[pl.ds(places[j] + (SUBLANES - 2 * j), SUBLANES), :], merged)
    return merged


def fetch_rows(lists, d, start, counts, src, mix, stages):
    half = SUBLANES // 2
    done = 0
    for count in counts:
        for first in range(done, done + count, half):
            places = [lists[d, start + first + j] for j in range(half)]
            mix[2 * first : 2 * first + SUBLANES, :] = pick_rows(src, places)
        done += count
    done = 0
    for stage, count in zip(stages, counts):
        stage[d, :count, :LANES] = mix[pl.ds(2 * done, count, stride=2), :].astype(BF16)
        stage[d, :count, LANES:] = mix[pl.ds(2 * done + 1, count, stride=2), :].astype(BF16)
        done += count


def widen_rows(x_ref, src):
    local = x_ref.shape[0]

    def widen(c, carry):
        row = pl.multiple_of(c * LANES, LANES)
        place = pl.multiple_of(2 * row + SUBLANES, SUBLANES)
        src[pl.ds(place, LANES, stride=2), :] = x_ref[pl.ds(row, LANES), :LANES].astype(F32)
        src[pl.ds(place + 1, LANES, stride=2), :] = x_ref[pl.ds(row, LANES), LANES:].astype(F32)
        return carry

    lax.fori_loop(0, local // LANES, widen, 0)


def send_kernel(
    place_ref, x_hbm, list_ref, out, hot_ref, count_ref, key_ref, x_ref, src, mix, stage, list_s, sem,
    *, groups, shards, first,
):
    devices = groups * shards
    chunks = place_ref.shape[0]
    local, width = x_ref.shape
    per = local // devices
    rows_in = pltpu.make_async_copy(x_hbm, x_ref, sem.at[0])
    rows_in.start()
    placement = place_ref[...].astype(F32)
    block = floor_div(placement, local)
    within = placement - block * local
    outer = floor_div(block, groups)
    target = (block - outer * groups) * shards + outer
    high = floor_div(within, LANES)
    low = within - high * LANES
    ids = lax.broadcasted_iota(jnp.int32, (devices, LANES), 0).astype(F32)
    for c in range(chunks):
        hot = (ids == target[c : c + 1, :]).astype(F32)
        hot_ref[:, c * LANES : (c + 1) * LANES] = hot.astype(BF16)
    before = lax.broadcasted_iota(jnp.int32, (LANES, LANES), 0) < lax.broadcasted_iota(
        jnp.int32, (LANES, LANES), 1
    )
    prefix = jnp.concatenate(
        [before.astype(F32), jnp.ones((LANES, LANES), F32)], axis=1
    ).astype(BF16)
    for c in range(chunks):
        count_ref[c * devices : (c + 1) * devices, :] = jnp.dot(
            hot_ref[:, c * LANES : (c + 1) * LANES], prefix, preferred_element_type=F32
        )
    carry = jnp.zeros((devices, LANES), F32)
    wide = list_ref.shape[1] // LANES
    order = lax.broadcasted_iota(jnp.int32, (devices, wide * LANES), 1).astype(F32)
    passed = jnp.zeros((devices, wide * LANES), F32)
    slots = lax.broadcasted_iota(jnp.int32, (per, LANES), 0).astype(F32).astype(BF16)
    lane = lax.broadcasted_iota(jnp.int32, (1, LANES), 1).astype(F32)
    zero = jnp.zeros((per, LANES), BF16)
    for c in range(chunks):
        counts = count_ref[c * devices : (c + 1) * devices, :]
        hot = hot_ref[:, c * LANES : (c + 1) * LANES].astype(F32)
        rank = jnp.sum(hot * (counts[:, :LANES] + carry), axis=0, keepdims=True)
        carry = carry + counts[:, LANES:]
        passed = passed + (jnp.concatenate([carry] * wide, axis=1) <= order).astype(F32)
        chosen = slots == jnp.broadcast_to(rank, (per, LANES)).astype(BF16)
        values = (high[c : c + 1, :], low[c : c + 1, :], lane)
        for k, value in enumerate(values):
            key_ref[k * per : (k + 1) * per, c * LANES : (c + 1) * LANES] = jnp.where(
                chosen, jnp.broadcast_to(value, (per, LANES)).astype(BF16), zero
            )
    codes = lax.dot_general(hot_ref[...], key_ref[...], NT, preferred_element_type=F32)
    source = 2.0 * (passed[:, :per] * LANES + codes[:, 2 * per :])
    list_ref[...] = jnp.zeros_like(list_ref)
    list_ref[:, :per] = source.astype(jnp.int32)
    lists_in = pltpu.make_async_copy(list_ref, list_s, sem.at[1])
    lists_in.start()
    line = lax.broadcasted_iota(jnp.int32, (TAIL, per), 0)
    label_high, label_low = codes[:, :per], codes[:, per : 2 * per]
    stage[:, first:, :] = jnp.zeros((devices, TAIL, width), BF16)
    for d in range(devices):
        tail = jnp.where(line == 0, label_high[d : d + 1], jnp.where(line == 1, label_low[d : d + 1], 0.0))
        stage[d, first:, :per] = tail.astype(BF16)
    rows_in.wait()
    widen_rows(x_ref, src)
    lists_in.wait()
    copies = []
    group = devices // sem.shape[0]
    for g in range(sem.shape[0]):
        for d in range(g * group, (g + 1) * group):
            own = mix.at[pl.ds(d % 2 * 2 * first, 2 * first)]
            fetch_rows(list_s, d, 0, (first,), src, own, (stage,))
        part = pl.ds(g * group, group)
        copies.append(pltpu.make_async_copy(stage.at[part], out.at[part], sem.at[g]))
        copies[-1].start()
    for copy in copies:
        copy.wait()


def send_first(placement, rows, groups, shards, first):
    devices = groups * shards
    local, width = rows.shape
    per = local // devices
    padded = -(-per // LANES) * LANES
    chunks = local // LANES
    vmem = pl.BlockSpec(memory_space=pltpu.VMEM)
    hbm = pl.BlockSpec(memory_space=pl.ANY)
    return pl.pallas_call(
        functools.partial(send_kernel, groups=groups, shards=shards, first=first),
        in_specs=[vmem, hbm],
        out_specs=(vmem, hbm),
        out_shape=(
            jax.ShapeDtypeStruct((devices, padded), jnp.int32),
            jax.ShapeDtypeStruct((devices, first + TAIL, width), BF16),
        ),
        scratch_shapes=[
            pltpu.VMEM((devices, local), BF16),
            pltpu.VMEM((chunks * devices, 2 * LANES), F32),
            pltpu.VMEM((3 * per, local), BF16),
            pltpu.VMEM((local, width), BF16),
            pltpu.VMEM((2 * (local + SUBLANES), LANES), F32),
            pltpu.VMEM((4 * first, LANES), F32),
            pltpu.VMEM((devices, first + TAIL, width), BF16),
            pltpu.SMEM((devices, padded), jnp.int32),
            pltpu.SemaphoreType.DMA((8,)),
        ],
        compiler_params=params(),
        name="send_first",
    )(placement.reshape(chunks, LANES), rows)


def rest_kernel(list_ref, x_ref, one, two, src, mix, *, first):
    widen_rows(x_ref, src)

    def fetch(d, carry):
        fetch_rows(list_ref, d, first, (one.shape[1], two.shape[1]), src, mix, (one, two))
        return carry

    lax.fori_loop(0, list_ref.shape[0], fetch, 0)


def send_rest(lists, rows, first, counts):
    local, width = rows.shape
    devices = lists.shape[0]
    return pl.pallas_call(
        functools.partial(rest_kernel, first=first),
        in_specs=[pl.BlockSpec(memory_space=pltpu.SMEM), pl.BlockSpec(memory_space=pltpu.VMEM)],
        out_shape=[jax.ShapeDtypeStruct((devices, n, width), BF16) for n in counts],
        scratch_shapes=[
            pltpu.VMEM((2 * (local + SUBLANES), LANES), F32),
            pltpu.VMEM((2 * sum(counts), LANES), F32),
        ],
        compiler_params=params(),
        cost_estimate=pl.CostEstimate(
            flops=2_000_000 * devices * sum(counts), bytes_accessed=6_000_000, transcendentals=0
        ),
        name="send_rest",
    )(lists, rows)


def slice_weights(standard, feeder_t, logit_t, sharp_ref, offset_ref, logit_ref, weight_ref, total_ref):
    heads = sharp_ref.shape[0]
    slices = offset_ref.shape[1]
    middle = lax.dot_general(feeder_t[...], standard, NT, preferred_element_type=F32).astype(BF16)
    logit_ref[...] = jnp.dot(logit_t[...], middle, preferred_element_type=F32)
    sharp = jnp.broadcast_to(sharp_ref[...], (heads, LANES))
    for start in range(0, weight_ref.shape[1], LANES):
        lanes = pl.ds(start, LANES)
        top = None
        for m in range(slices):
            value = (logit_ref[m * heads : (m + 1) * heads, lanes] + offset_ref[0, m]) * sharp
            top = value if top is None else jnp.maximum(top, value)
        total = None
        for m in range(slices):
            value = (logit_ref[m * heads : (m + 1) * heads, lanes] + offset_ref[0, m]) * sharp
            value = jnp.exp2(value - top)
            logit_ref[m * heads : (m + 1) * heads, lanes] = value
            total = value if total is None else total + value
        scale = 1.0 / total
        for m in range(slices):
            value = logit_ref[m * heads : (m + 1) * heads, lanes] * scale
            weight_ref[m * heads : (m + 1) * heads, lanes] = value.astype(BF16)
            if total_ref is not None:
                total_ref[m * heads : (m + 1) * heads, :] += value


def head_mask(rows, width, heads):
    row_head = lax.broadcasted_iota(jnp.int32, (rows, width), 0) % heads
    return row_head == lax.broadcasted_iota(jnp.int32, (rows, width), 1) // (width // heads)


def repeat_heads(value, width, dims):
    feature = value.shape[dims[0][0][0]]
    pick = lax.broadcasted_iota(jnp.int32, (feature, width), 1) % feature == lax.broadcasted_iota(
        jnp.int32, (feature, width), 0
    )
    return lax.dot_general(
        value, pick.astype(F32), dims, precision=lax.Precision.HIGHEST, preferred_element_type=F32
    )


def sums_kernel(
    x_ref, gain, bias, attribute, feeder_t, partition, sharp_ref, offset_ref,
    packed_ref, logit_t, logit_ref, weight_ref, total_ref, numer_ref,
):
    step = pl.program_id(0)
    heads = sharp_ref.shape[0]
    rows, width = numer_ref.shape
    slices = rows // heads

    @pl.when(step == 0)
    def _():
        total_ref[...] = jnp.zeros_like(total_ref)
        numer_ref[...] = jnp.zeros_like(numer_ref)
        wide = repeat_heads(partition[...].astype(F32), width, TN)
        wide = jnp.broadcast_to(wide[:, None, :], (slices, heads, width))
        logit_t[...] = jnp.where(
            head_mask(rows, width, heads), wide.reshape(rows, width), 0.0
        ).astype(BF16)

    standard = norm_rows(x_ref[...].astype(F32), gain[...], bias[...]).astype(BF16)
    features = jnp.dot(standard, attribute[...], preferred_element_type=F32).astype(BF16)
    slice_weights(
        standard, feeder_t, logit_t, sharp_ref, offset_ref, logit_ref, weight_ref, total_ref
    )
    numer_ref[...] += jnp.dot(weight_ref[...], features, preferred_element_type=F32)

    @pl.when(step == pl.num_programs(0) - 1)
    def _():
        own = jnp.where(head_mask(rows, width, heads), numer_ref[...], 0.0)
        packed_ref[:, :width] = jnp.sum(own.reshape(slices, heads, width), axis=1)
        sums = jnp.sum(total_ref[...], axis=1, keepdims=True)
        lane = lax.broadcasted_iota(jnp.int32, (rows, LANES), 1)
        row_head = lax.broadcasted_iota(jnp.int32, (rows, LANES), 0) % heads
        own = jnp.where(row_head == lane, sums, 0.0)
        packed_ref[:, width:] = jnp.sum(own.reshape(slices, heads, LANES), axis=1)


def local_sums(x, gain, bias, attribute, feeder_t, partition, sharp, offset, block):
    local, width = x.shape
    heads = sharp.shape[0]
    slices = partition.shape[1]
    rows = slices * heads
    return pl.pallas_call(
        sums_kernel,
        grid=(local // block,),
        in_specs=[
            pl.BlockSpec((block, width), lambda i: (i, 0)),
            whole(gain.shape), whole(bias.shape), whole(attribute.shape), whole(feeder_t.shape),
            whole(partition.shape), whole(sharp.shape),
            pl.BlockSpec(memory_space=pltpu.SMEM),
        ],
        out_specs=(whole((slices, width + LANES)), whole((rows, width))),
        out_shape=(
            jax.ShapeDtypeStruct((slices, width + LANES), F32),
            jax.ShapeDtypeStruct((rows, width), BF16),
        ),
        scratch_shapes=[
            pltpu.VMEM((rows, block), F32),
            pltpu.VMEM((rows, block), BF16),
            pltpu.VMEM((rows, LANES), F32),
            pltpu.VMEM((rows, width), F32),
        ],
        compiler_params=params(),
        cost_estimate=pl.CostEstimate(flops=5_000_000_000, bytes_accessed=4_000_000, transcendentals=3_000_000),
        name="local_sums",
    )(x, gain, bias, attribute, feeder_t, partition, sharp, offset)


def attention_kernel(packed_ref, question, lookup, content, mix_t, *, heads):
    highest = lax.Precision.HIGHEST
    slices = packed_ref.shape[0]
    width = packed_ref.shape[1] - LANES
    feature = width // heads
    rows = slices * heads
    spread = (
        lax.broadcasted_iota(jnp.int32, (LANES, width), 0)
        == lax.broadcasted_iota(jnp.int32, (LANES, width), 1) // feature
    ).astype(F32)
    totals = jnp.dot(packed_ref[:, width:], spread, precision=highest, preferred_element_type=F32)
    token = packed_ref[:, :width] / (totals + 1e-05)
    own = (
        lax.broadcasted_iota(jnp.int32, (width, width), 0) // feature
        == lax.broadcasted_iota(jnp.int32, (width, width), 1) // feature
    )

    def per_head(weight):
        wide = repeat_heads(weight[...], width, NN)
        tiled = jnp.broadcast_to(wide[None], (heads, feature, width)).reshape(width, width)
        return jnp.dot(token, jnp.where(own, tiled, 0.0), precision=highest, preferred_element_type=F32)

    query = per_head(question)
    key = per_head(lookup)
    value = per_head(content)
    mask = head_mask(rows, width, heads)
    query = jnp.broadcast_to(query[:, None, :], (slices, heads, width)).reshape(rows, width)
    query = jnp.where(mask, query, 0.0)
    scores = lax.dot_general(query, key, NT, precision=highest, preferred_element_type=F32)
    scores = scores * (1.0 / math.sqrt(feature))
    scores = jnp.exp(scores - jnp.max(scores, axis=-1, keepdims=True))
    attention = scores / jnp.sum(scores, axis=-1, keepdims=True)
    mixed = jnp.dot(attention, value, precision=highest, preferred_element_type=F32)
    mix_t[...] = jnp.where(mask, mixed, 0.0).T.astype(BF16)


def slice_attention(packed, question, lookup, content, heads):
    slices = packed.shape[0]
    width = packed.shape[1] - LANES
    return pl.pallas_call(
        functools.partial(attention_kernel, heads=heads),
        out_shape=jax.ShapeDtypeStruct((width, slices * heads), BF16),
        compiler_params=params(),
        name="slice_attention",
    )(packed, question, lookup, content)


def finish_kernel(
    pos_hbm, x_ref, gain, bias, feeder_t, logit_t, sharp_ref, offset_ref, mix_t, emitted, emitted_offset,
    gain2, bias2, entry, entry_offset, leave, leave_offset, *refs, start, per, follows, last,
):
    refs = list(refs)
    before = refs.pop(0) if follows else None
    out_ref, logit_ref, weight_ref, res, dst, pos_ref, sem, pos_sem = refs[:8]
    step = pl.program_id(0)
    sources = x_ref.shape[0]
    block = sources * per
    local = dst.shape[0] // 2

    slots_in = pltpu.make_async_copy(
        pos_hbm.at[pl.ds(pl.multiple_of(step * sources, 8), sources)], pos_ref, pos_sem.at[0]
    )
    slots_in.start()

    def handover(inward):
        if inward:
            return pltpu.make_async_copy(before, dst, sem.at[0])
        return pltpu.make_async_copy(dst, out_ref, sem.at[0])

    if follows:

        @pl.when(step == 0)
        def _():
            handover(True).start()

    x = jnp.concatenate([x_ref[s, :per, :] for s in range(sources)], axis=0).astype(F32)
    standard = norm_rows(x, gain[...], bias[...]).astype(BF16)
    slice_weights(standard, feeder_t, logit_t, sharp_ref, offset_ref, logit_ref, weight_ref, None)
    blended_t = jnp.dot(mix_t[...], weight_ref[...], preferred_element_type=F32)
    blended = blended_t.T.astype(BF16)
    hidden = x + jnp.dot(blended, emitted[...], preferred_element_type=F32) + emitted_offset[...]
    normed = norm_rows(hidden, gain2[...], bias2[...]).astype(BF16)
    inner = jnp.dot(normed, entry[...], preferred_element_type=F32) + entry_offset[...]
    active = (inner * (1.0 + lax.erf(inner * math.sqrt(0.5)))).astype(BF16)
    leaving = jnp.dot(active, leave[...], preferred_element_type=F32)
    result = hidden + 0.5 * leaving + leave_offset[...]
    res[:block, :] = result[:, :LANES]
    res[block:, :] = result[:, LANES:]
    if follows:

        @pl.when(step == 0)
        def _():
            handover(True).wait()

    slots_in.wait()
    for source in range(sources):
        for j in range(per):
            slot = pos_ref[source, start + j]
            row = source * per + j
            dst[pl.ds(slot, 1), :] = res[row : row + 1, :]
            dst[pl.ds(slot + local, 1), :] = res[row + block : row + block + 1, :]

    @pl.when(step == pl.num_programs(0) - 1)
    def _():
        if not last:
            handover(False).start()
            handover(False).wait()
        else:
            stage = refs[8]
            parts = sem.shape[0]
            size = local // parts
            copies = []
            for q in range(parts):

                def narrow(c, carry, q=q):
                    row = pl.multiple_of(q * size + c * LANES, LANES)
                    stage[pl.ds(row, LANES), :LANES] = dst[pl.ds(row, LANES), :].astype(BF16)
                    stage[pl.ds(row, LANES), LANES:] = dst[pl.ds(row + local, LANES), :].astype(BF16)
                    return carry

                lax.fori_loop(0, size // LANES, narrow, 0)
                rows = pl.ds(q * size, size)
                copies.append(pltpu.make_async_copy(stage.at[rows], out_ref.at[rows], sem.at[q]))
                copies[-1].start()
            for copy in copies:
                copy.wait()


def finish_rows(positions, arrived, weights, offset, mix_t, rest, before, local, start, per, last):
    devices, stride, width = arrived.shape
    rows = mix_t.shape[1]
    sources = max(
        k for k in range(8, devices + 1, 8)
        if devices % k == 0 and k * per <= BLOCK and k * per % LANES == 0
    )
    block = sources * per
    follows = before is not None
    shape = (local, width) if last else (2 * local, LANES)
    return pl.pallas_call(
        functools.partial(finish_kernel, start=start, per=per, follows=follows, last=last),
        grid=(devices // sources,),
        in_specs=[
            pl.BlockSpec(memory_space=pl.ANY),
            pl.BlockSpec((sources, stride, width), lambda i: (i, 0, 0)),
            *[whole(w.shape) for w in weights],
            pl.BlockSpec(memory_space=pltpu.SMEM),
            whole(mix_t.shape),
            *[whole(w.shape) for w in rest],
            *([pl.BlockSpec(memory_space=pl.ANY)] if follows else []),
        ],
        out_specs=pl.BlockSpec(memory_space=pl.ANY),
        out_shape=jax.ShapeDtypeStruct(shape, BF16 if last else F32),
        scratch_shapes=[
            pltpu.VMEM((rows, block), F32),
            pltpu.VMEM((rows, block), BF16),
            pltpu.VMEM((2 * block, LANES), F32),
            pltpu.VMEM((2 * local, LANES), F32),
            pltpu.SMEM((sources, positions.shape[1]), jnp.int32),
            pltpu.SemaphoreType.DMA((4 if last else 1,)),
            pltpu.SemaphoreType.DMA((1,)),
            *([pltpu.VMEM((local, width), BF16)] if last else []),
        ],
        compiler_params=params(),
        cost_estimate=pl.CostEstimate(
            flops=2_000_000 * devices * per, bytes_accessed=8_000_000, transcendentals=1000 * devices * per
        ),
    )(positions, arrived, *weights, offset, mix_t, *rest, *([before] if follows else []))


def sum_plane(value, shards):
    step = 1
    while step < shards:
        value = value + lax.ppermute(value, "pts", [(i, i ^ step) for i in range(shards)])
        step *= 2
    return value


def sum_head(value, groups):
    others = [lax.ppermute(value, "head", [(i, i ^ k) for i in range(groups)]) for k in range(1, groups)]
    for other in others:
        value = value + other
    return value


def body(
    layer_inputs_trainorder,
    inference_placement,
    initial_layernorm_gain,
    initial_layernorm_offset,
    attribute_projection,
    assignment_feeder_projection,
    partition_projection,
    partition_offset,
    softmax_sharpness,
    partition_question_map,
    partition_lookup_map,
    partition_content_map,
    emitted_projection,
    emitted_offset,
    latter_layernorm_gain,
    latter_layernorm_offset,
    perceptron_entry_map,
    perceptron_entry_offset,
    perceptron_exit_map,
    perceptron_exit_offset,
):
    groups = lax.axis_size("head")
    shards = lax.axis_size("pts")
    devices = groups * shards
    local, width = layer_inputs_trainorder.shape
    feature, _ = partition_projection.shape
    heads = width // feature
    per = local // devices
    block = 768 if local % 768 == 0 else LANES
    first = per // 2 // 8 * 8
    second = per // 3 // 8 * 8
    third = per - first - second

    def exchange(rows):
        return lax.all_to_all(rows, ("head", "pts"), split_axis=0, concat_axis=0, tiled=True)

    mates = [
        lax.ppermute(softmax_sharpness, "head", [(i, i ^ k) for i in range(groups)])
        for k in range(1, groups)
    ]
    lists, one = send_first(inference_placement, layer_inputs_trainorder, groups, shards, first)
    *mates, one = lax.optimization_barrier((*mates, one))
    arrived_one = exchange(one)
    two, three = send_rest(lists, layer_inputs_trainorder, first, (second, third))

    place = lax.axis_index("head")
    order = jnp.arange(groups)[:, None]
    sharp = jnp.where(order == place, softmax_sharpness[None], 0.0)
    for k, mate in enumerate(mates, 1):
        sharp = jnp.where(order == (place ^ k), mate[None], sharp)
    sharp = (LOG2E / sharp).reshape(heads, 1)
    gain = initial_layernorm_gain[None]
    bias = initial_layernorm_offset[None]
    feeder_t = assignment_feeder_projection.T
    offset = partition_offset[None]
    packed, logit_t = local_sums(
        layer_inputs_trainorder, gain, bias, attribute_projection, feeder_t, partition_projection, sharp,
        offset, block,
    )
    packed = sum_plane(packed, shards)
    _, arrived_one, two = lax.optimization_barrier((packed, arrived_one, two))
    arrived_two = exchange(two)
    packed = sum_head(packed, groups)

    codes = lax.optimization_barrier(arrived_one[:, first:, :])[:, :2, :].astype(F32)
    arrived_at = (codes[:, 0] * LANES + codes[:, 1]).astype(jnp.int32)
    mix_t = slice_attention(
        packed, partition_question_map, partition_lookup_map, partition_content_map, heads
    )
    weights = (gain, bias, feeder_t, logit_t, sharp)
    rest = (
        emitted_projection, emitted_offset[None], latter_layernorm_gain[None], latter_layernorm_offset[None],
        perceptron_entry_map, perceptron_entry_offset[None],
        perceptron_exit_map, perceptron_exit_offset[None],
    )
    served = finish_rows(
        arrived_at, arrived_one, weights, offset, mix_t, rest, None, local, 0, first, False
    )
    served, arrived_two, three = lax.optimization_barrier((served, arrived_two, three))
    arrived_three = exchange(three)
    served = finish_rows(
        arrived_at, arrived_two, weights, offset, mix_t, rest, served, local, first, second, False
    )
    served = finish_rows(
        arrived_at, arrived_three, weights, offset, mix_t, rest, served, local, first + second, third, True
    )
    return served[None]


def solution(mesh):
    rows = P(("head", "pts"))
    placed = (P(("head", "pts"), None), rows, *[P()] * 6, P("head"), *[P()] * 11)

    return jax.shard_map(body, mesh=mesh, in_specs=placed, out_specs=P("pts", "head", None), check_vma=False)
```
